128 devices in a mesh: span: 8 (over y, core), height: 4 (over x), depth: 4 (over z).
Axes of the slice: x: 4, y: 4, z: 4, core: 2. Of those that a mesh axis runs over, the one named last changes fastest.
Arguments:
- load: float32 [8, 128, 64, 512], P(None, 'span', 'height', 'depth'), may hold values from -6 to 6
- phase: float32 [128, 64, 512], P('span', 'height', 'depth'), may hold values from 0.1 to 1
- void: int32 [16, 8, 64], P('span', 'height', 'depth'), may hold values from 0 to 1, as said below
- owner: int32 [16, 8, 64], P('span', 'height', 'depth'), may hold values from 0 to 7, as said below
- precond: bfloat16 [2048, 512, 512], P(('span', 'height', 'depth')), may hold values from -1 to 2, as said below
Outputs:
- displacement: float32 [8, 128, 64, 512], P(None, 'span', 'height', 'depth')
- sensitivity: float32 [128, 64, 512], P('span', 'height', 'depth')
- phase_next: float32 [128, 64, 512], P('span', 'height', 'depth')
The draws below stay inside these ranges and needn't reach their ends.
Inputs may be any that keep to these rules, and one draw needn't show every extreme that they name: `void`: each device's block of 16 x 16 x 128 cells holds at most 16 solid bricks; some device holds exactly 16. `owner`: among the solid bricks of one device at most 2 name any one value; on some device every value is named by exactly 2 solid bricks. Values of void bricks carry no meaning. `precond`: every block is symmetric with a positive diagonal that dominates each row.
All inputs are finite; a program needn't handle non-finite values.
Results may differ from the reference program's by a relative error of at most 0.0021.
Values may be sent and summed in bfloat16 or wider, within the bound.
A program may use at most 128 MiB of HBM per device.

```python
import jax
import jax.numpy as jnp
from jax import lax

BE = 8
CX = 16
CY = 16
CZ = 128
NLOAD = 8
ITERS = 2
SWEEPS = 2
BC = 512
NBD = 64
OWN = 16
CAP = 2
SLOTS = 2048
NX = 128
NY = 64
NZ = 512
N_SPAN = 8
N_HEIGHT = 4
N_DEPTH = 4


def brick_plan(key):
    key = jax.random.fold_in(key, 7)
    span_count = NX // CX
    height_count = NY // CY
    depth_count = NZ // CZ
    device_count = span_count * height_count * depth_count
    capacity = OWN // span_count
    first, second, third, fourth = jax.random.split(key, 4)
    counts = jax.random.randint(first, (device_count,), OWN // 4, OWN + 1)
    chosen = jax.random.randint(second, (), 0, device_count)
    counts = jnp.where(jnp.arange(device_count) == chosen, OWN, counts)
    scores = jax.random.randint(third, (device_count, NBD), 0, 1 << 20) * NBD + jnp.arange(NBD, dtype=jnp.int32)[None, :]
    ordering = jnp.argsort(scores, axis=1)
    position = jnp.argsort(ordering, axis=1)
    solid = (position < counts[:, None]).astype(jnp.int32)
    before = jnp.cumsum(solid, axis=1) - solid
    offsets = jax.random.randint(fourth, (device_count,), 0, span_count)
    span_index = jnp.arange(device_count, dtype=jnp.int32) // (height_count * depth_count)
    owners = (span_index[:, None] + offsets[:, None] + before // capacity) % span_count

    def to_grid(values):
        g = values.reshape(span_count, height_count, depth_count, CX // BE, CY // BE, CZ // BE)
        g = g.transpose(0, 3, 1, 4, 2, 5)
        return g.reshape(NX // BE, NY // BE, NZ // BE).astype(jnp.int32)
    return (to_grid(1 - solid), to_grid(owners))


def draw_void(key, part):
    return brick_plan(key)[0]


def draw_owner(key, part):
    return brick_plan(key)[1]


def draw_precond(key, part):
    key = jax.random.fold_in(key, 11)

    def one_block(index):
        block_key = jax.random.fold_in(key, index)
        first, second = jax.random.split(block_key)
        raw = jax.random.normal(first, (BC, BC), jnp.float32) * (0.9 / BC)
        symmetric = 0.5 * (raw + raw.T)
        diagonal = jax.random.uniform(second, (BC,), jnp.float32, 1.0, 2.0)
        identity = jnp.eye(BC, dtype=jnp.float32)
        return (symmetric * (1.0 - identity) + diagonal[:, None] * identity).astype(jnp.bfloat16)
    return jax.lax.map(one_block, jnp.arange(SLOTS, dtype=jnp.int32))


def steps_of(rng, shape, shards, smallest, top_value):
    factor_of = 1.0
    for dim, shards_of in shards:
        steps = jax.random.uniform(jax.random.fold_in(jax.random.fold_in(rng, 6), dim), (shards_of,), jnp.float32, smallest / len(shards), top_value / len(shards))
        factor_of = factor_of * jnp.repeat(jnp.exp(steps), shape[dim] // shards_of).reshape((-1,) + (1,) * (len(shape) - 1 - dim))
    return factor_of


def gaussian(key, dims, scale, reach, cuts=(), kind=jnp.bfloat16):
    entries = scale * jax.random.normal(key, dims, jnp.float32)
    if cuts:
        entries = entries * steps_of(key, dims, cuts, -0.22, 0.18)
    return jnp.clip(entries, -reach, reach).astype(kind)


def setup_inputs(seed: int = 0) -> dict:
    streams_of = jax.random.split(jax.random.key(seed), 6)
    load = gaussian(streams_of[0], (NLOAD, NX, NY, NZ), 1.0, 6.0, ((1, 8), (2, 4), (3, 4)), jnp.float32)
    phase = jnp.clip(0.1 + 0.9 * jax.random.uniform(streams_of[1], (NX, NY, NZ), jnp.float32) ** steps_of(streams_of[1], (NX, NY, NZ), ((0, 8), (1, 4), (2, 4)), -0.2, 0.2), 0.1, 1.0)
    void = draw_void(jax.random.fold_in(streams_of[5], 71), 0)
    owner = draw_owner(jax.random.fold_in(streams_of[5], 71), 0)
    precond = draw_precond(jax.random.fold_in(streams_of[5], 71), 0)
    return {"load": load, "phase": phase, "void": void, "owner": owner, "precond": precond}


void_stiffness = 0.001
spring_rate = 0.05
time_step = 0.5
interface_weight = 0.5
epsilon_peak = 1e-6


def pad_three(field):
    return jnp.pad(field, [(0, 0)] * (field.ndim - 3) + [(1, 1)] * 3)


def neighbours(padded):
    return [padded[..., 2:, 1:-1, 1:-1], padded[..., :-2, 1:-1, 1:-1],
            padded[..., 1:-1, 2:, 1:-1], padded[..., 1:-1, :-2, 1:-1],
            padded[..., 1:-1, 1:-1, 2:], padded[..., 1:-1, 1:-1, :-2]]


def cells_of(bricks):
    expanded = jnp.broadcast_to(bricks[:, None, :, None, :, None], (bricks.shape[0], BE, bricks.shape[1], BE, bricks.shape[2], BE))
    return expanded.reshape(bricks.shape[0] * BE, bricks.shape[1] * BE, bricks.shape[2] * BE)


def local_order(grid):
    g = grid.reshape(N_SPAN, CX // BE, N_HEIGHT, CY // BE, N_DEPTH, CZ // BE).transpose(0, 2, 4, 1, 3, 5)
    return g.reshape(N_SPAN * N_HEIGHT * N_DEPTH, NBD)


def to_device_bricks(field):
    loads = field.shape[0]
    f = field.reshape(loads, N_SPAN, CX // BE, BE, N_HEIGHT, CY // BE, BE, N_DEPTH, CZ // BE, BE)
    f = f.transpose(1, 4, 7, 2, 5, 8, 0, 3, 6, 9)
    return f.reshape(N_SPAN * N_HEIGHT * N_DEPTH * NBD, loads, BC)


def from_device_bricks(bricks):
    loads = bricks.shape[1]
    f = bricks.reshape(N_SPAN, N_HEIGHT, N_DEPTH, CX // BE, CY // BE, CZ // BE, loads, BE, BE, BE)
    f = f.transpose(6, 0, 3, 7, 1, 4, 8, 2, 5, 9)
    return f.reshape(loads, NX, NY, NZ)


def slot_table(void, owner):
    solid = 1 - local_order(void)
    owned = local_order(owner)
    columns = jnp.arange(N_SPAN, dtype=jnp.int32)
    onehot = (owned[:, :, None] == columns[None, None, :]).astype(jnp.int32) * solid[:, :, None]
    before = jnp.cumsum(onehot, axis=1) - onehot
    rank = jnp.sum(before * onehot, axis=2)
    device_ids = jnp.arange(N_SPAN * N_HEIGHT * N_DEPTH, dtype=jnp.int32)
    cross = device_ids % (N_HEIGHT * N_DEPTH)
    source = device_ids // (N_HEIGHT * N_DEPTH)
    owner_device = owned * (N_HEIGHT * N_DEPTH) + cross[:, None]
    slot = owner_device * OWN + source[:, None] * CAP + rank
    slot = jnp.where(solid == 1, slot, SLOTS).astype(jnp.int32)
    return slot.reshape(-1), solid.reshape(-1)


def precondition(residual, precond, slot, solid):
    bricks = to_device_bricks(residual.astype(jnp.bfloat16))
    loads = bricks.shape[1]
    filled = jnp.zeros((SLOTS, loads, BC), jnp.bfloat16).at[slot].set(bricks, mode="drop")
    blocks = precond.reshape(N_SPAN * N_HEIGHT * N_DEPTH, OWN, BC, BC)
    inputs = filled.reshape(N_SPAN * N_HEIGHT * N_DEPTH, OWN, loads, BC)

    def apply_device(pair):
        return jnp.einsum("sij,slj->sli", pair[0].astype(jnp.float32), pair[1].astype(jnp.float32))

    images = lax.map(apply_device, (blocks, inputs)).reshape(SLOTS, loads, BC)
    safe = jnp.minimum(slot, SLOTS - 1).astype(jnp.int32)
    result = images[safe] * solid.astype(jnp.float32)[:, None, None]
    return from_device_bricks(result)


def reference(load, phase, void, owner, precond):
    cell_mask = cells_of((1 - void).astype(jnp.float32))
    stiffness = void_stiffness + (1.0 - void_stiffness) * phase ** 3
    near_mask = neighbours(pad_three(cell_mask))
    near_stiff = neighbours(pad_three(cell_mask * stiffness))
    weights = [cell_mask * 0.5 * (nm * stiffness + nk) for nm, nk in zip(near_mask, near_stiff)]

    def operate(field):
        total = cell_mask * spring_rate * field
        for weight, near in zip(weights, neighbours(pad_three(field))):
            total = total + weight * (field - near)
        return total

    slot, solid = slot_table(void, owner)
    right_side = cell_mask[None] * load
    solution = jnp.zeros_like(right_side)
    residual = right_side
    search = precondition(residual, precond, slot, solid)
    norm_now = jnp.sum(residual * search, axis=(1, 2, 3))
    direction = search
    for iteration in range(ITERS):
        image = operate(direction)
        step_size = norm_now / jnp.sum(direction * image, axis=(1, 2, 3))
        solution = solution + step_size[:, None, None, None] * direction
        residual = residual - step_size[:, None, None, None] * image
        if iteration + 1 < ITERS:
            search = precondition(residual, precond, slot, solid)
            norm_next = jnp.sum(residual * search, axis=(1, 2, 3))
            direction = search + (norm_next / norm_now)[:, None, None, None] * direction
            norm_now = norm_next
    energy = jnp.zeros_like(phase)
    for mask_near, near in zip(near_mask, neighbours(pad_three(solution))):
        energy = energy + mask_near * jnp.sum((solution - near) ** 2, axis=0)
    sensitivity = -1.5 * (1.0 - void_stiffness) * phase ** 2 * cell_mask * energy
    peak_value = jnp.max(-sensitivity)
    drive = phase / time_step - 0.5 * phase * (1.0 - phase) * (1.0 - 2.0 * phase) - sensitivity / (peak_value + epsilon_peak)
    inverse = 1.0 / (1.0 / time_step + 6.0 * interface_weight)
    current = phase
    for sweep_index in range(SWEEPS):
        beside_all = neighbours(pad_three(current))
        current = (drive + interface_weight * (beside_all[0] + beside_all[1] + beside_all[2] + beside_all[3] + beside_all[4] + beside_all[5])) * inverse
    return solution, sensitivity, current
```

```python
import functools

import jax
import jax.numpy as jnp
from jax import lax
from jax.experimental import pallas as pl
from jax.experimental.pallas import tpu as pltpu
from jax.sharding import PartitionSpec as P

AXES = ("span", "height", "depth")
MESH = pl.DeviceIdType.MESH
F32 = jnp.float32
BF16 = jnp.bfloat16

void_stiffness = 0.001
spring_rate = 0.05
time_step = 0.5
interface_weight = 0.5
epsilon_peak = 1e-06
inverse = 1.0 / (1.0 / time_step + 6.0 * interface_weight)

PITCH = 264

PARTNERS = ((0, 1), (1, 0), (3, 0), (1, 1), (3, 1), (2, 0), (2, 1))
FAR_FIRST = (5, 6, 1, 2, 3, 4, 0)


def block_transpose(rows):
    lane_block = lax.broadcasted_iota(jnp.int32, (8, 128), 1) // 8
    rows = [pltpu.roll(r, 8 * t, 1) if t else r for t, r in enumerate(rows)]
    for bit in (1, 2, 4, 8):
        taken = (lane_block % (2 * bit)) >= bit
        rows = [jnp.where(taken, rows[(t + bit) % 16], rows[t]) for t in range(16)]
    out = []
    for s in range(16):
        r = rows[(16 - s) % 16]
        out.append(pltpu.roll(r, 128 - 8 * s, 1) if s else r)
    return out


def kernel(
    sizes,
    load_hbm, phase_hbm, void_hbm, owner_hbm, precond_hbm,
    disp_hbm, sens_hbm, next_hbm,
    load_v, void_v, owner_v, pre_v, sel, ez, mrow, lb, vs, gbuf,
    send_a, recv_a, send_r, recv_r, field, image, hz_s, hz_r, hz_m, xfield, dx,
    ext, sf_s, sf_r, sf_m, dco, wx, wyp, wym, wzl, wze, base, hpart, erow, sens, nxt, ar_s, ar_r,
    in_sem, pre_sem, out_sem, a2a_ss, a2a_rs, ret_ss, ret_rs, halo_ss, halo_rs,
    sf_ss, sf_rs, ar_ss, ar_rs,
):
    n_span, n_height, n_depth = sizes
    S, H, D = (lax.axis_index(a) for a in AXES)
    yy, core = S // 2, S % 2
    lane = lax.broadcasted_iota(jnp.int32, (8, 128), 1)

    def towards(dy, dc):
        return lax.rem(yy + dy, 4) * 2 + (1 - core if dc else core)

    def back(dy, dc):
        return lax.rem(yy + 4 - dy, 4) * 2 + (1 - core if dc else core)

    load_in = [
        pltpu.make_async_copy(
            load_hbm.at[pl.ds(l * 256, 256)], load_v.at[pl.ds(l * PITCH, 256)], in_sem.at[l]
        )
        for l in range(8)
    ]
    void_in = pltpu.make_async_copy(void_hbm, void_v, in_sem.at[8])
    owner_in = pltpu.make_async_copy(owner_hbm, owner_v, in_sem.at[9])
    phase_in = pltpu.make_async_copy(phase_hbm, ext.at[1, pl.ds(16, 256)], in_sem.at[10])
    void_in.start()
    owner_in.start()
    for c in load_in:
        c.start()
    phase_in.start()

    barrier = pltpu.get_barrier_semaphore()
    for dy, dc in PARTNERS:
        pl.semaphore_signal(barrier, 1, device_id={"span": towards(dy, dc)}, device_id_type=MESH)
    for d in range(1, n_height):
        pl.semaphore_signal(
            barrier, 1, device_id={"height": lax.rem(H + d, n_height)}, device_id_type=MESH
        )
    for d in range(1, n_depth):
        pl.semaphore_signal(
            barrier, 1, device_id={"depth": lax.rem(D + d, n_depth)}, device_id_type=MESH
        )

    sources = [S] + [back(dy, dc) for dy, dc in PARTNERS]
    pre_in = [
        pltpu.make_async_copy(
            precond_hbm.at[pl.ds(src * 2, 2)], pre_v.at[pl.ds(src * 2, 2)], pre_sem.at[n]
        )
        for n, src in enumerate(sources)
    ]
    for c in pre_in:
        c.start()

    void_in.wait()
    owner_in.wait()
    o_row = lax.broadcasted_iota(jnp.int32, (8, 16), 0)
    onehots = []
    for bx in range(2):
        own2, solid2 = owner_v[bx], 1 - void_v[bx]
        for by in range(2):
            own_row = jnp.broadcast_to(own2[by : by + 1, :], (8, 16))
            sol_row = jnp.broadcast_to(solid2[by : by + 1, :], (8, 16))
            onehots.append(jnp.where((own_row == o_row) & (sol_row == 1), 1.0, 0.0))
    onehot = jnp.concatenate(onehots, axis=0)
    b_row = lax.broadcasted_iota(jnp.int32, (16, 128), 0)
    b_lane = lax.broadcasted_iota(jnp.int32, (16, 128), 1) // 8
    spread = jnp.concatenate(
        [
            jnp.where(b_row == b_lane, 1.0, 0.0),
            jnp.where(b_row < b_lane, 1.0, 0.0),
            jnp.ones((16, 128), F32),
        ],
        axis=1,
    )
    counted = jnp.dot(onehot, spread, preferred_element_type=F32)
    o_col = lax.broadcasted_iota(jnp.int32, (8, 128), 0).astype(F32)
    row_id = lax.broadcasted_iota(jnp.int32, (128, 128), 0).astype(F32)
    lane_row = lax.broadcasted_iota(jnp.int32, (1, 128), 1)
    previous = jnp.zeros((8, 128), F32)
    edge = jnp.full((1, 128), -1.0, F32)
    for c in range(4):
        here = counted[c * 8 : c * 8 + 8, 0:128]
        before = counted[c * 8 : c * 8 + 8, 128:256] + previous
        previous = previous + counted[c * 8 : c * 8 + 8, 256:384]
        solid = jnp.sum(here, axis=0, keepdims=True)
        slot = jnp.sum(here * (2.0 * o_col + before), axis=0, keepdims=True)
        code = jnp.where(solid > 0.5, slot * 8.0 + (lane_row % 8).astype(F32), -1.0)
        mrow[c : c + 1, :] = solid
        picked = jnp.where(row_id == code, 1.0, 0.0).astype(BF16)
        sel[0:128, c * 128 : (c + 1) * 128] = picked
        sel[128:256, c * 128 : (c + 1) * 128] = picked
        edge = jnp.where(lane_row % 8 == 2 * c, jnp.broadcast_to(code[:, 127:128], (1, 128)), edge)
        edge = jnp.where(lane_row % 8 == 2 * c + 1, jnp.broadcast_to(code[:, 0:1], (1, 128)), edge)
    picked = jnp.where(row_id == edge, 1.0, 0.0).astype(BF16)
    ez[0:128, :] = picked
    ez[128:256, :] = picked

    def halo_copies(it):
        f = field.at[it]
        inner = pl.ds(1, 16)
        copies = []
        for n, (axis, idx, size, src, dst) in enumerate(
            (
                ("span", S, n_span, f.at[16, inner], f.at[0, inner]),
                ("span", S, n_span, f.at[1, inner], f.at[17, inner]),
                ("height", H, n_height, f.at[inner, 16], f.at[inner, 0]),
                ("height", H, n_height, f.at[inner, 1], f.at[inner, 17]),
                ("depth", D, n_depth, hz_s.at[it], hz_r.at[it, 0]),
                ("depth", D, n_depth, hz_s.at[it], hz_r.at[it, 1]),
            )
        ):
            copies.append((axis, idx, size, n % 2, src, dst, halo_ss.at[it, n], halo_rs.at[it, n]))
        return copies

    def small_copies(e):
        f = ext.at[e]
        copies = []
        for n, (axis, idx, size, src, dst) in enumerate(
            (
                ("span", S, n_span, f.at[pl.ds(256, 16)], f.at[pl.ds(0, 16)]),
                ("span", S, n_span, f.at[pl.ds(16, 16)], f.at[pl.ds(272, 16)]),
                ("height", H, n_height, sf_s.at[e, 1], sf_r.at[e, 0]),
                ("height", H, n_height, sf_s.at[e, 0], sf_r.at[e, 1]),
                ("depth", D, n_depth, sf_s.at[e, 2, pl.ds(0, 8)], sf_r.at[e, 2, pl.ds(0, 8)]),
                ("depth", D, n_depth, sf_s.at[e, 2, pl.ds(0, 8)], sf_r.at[e, 2, pl.ds(8, 8)]),
            )
        ):
            copies.append((axis, idx, size, n % 2, src, dst, sf_ss.at[e, n], sf_rs.at[e, n]))
        return copies

    def make(copy):
        axis, idx, size, direction, src, dst, ss, rs = copy
        target = idx + 1 if direction == 0 else idx - 1
        return pltpu.make_async_remote_copy(
            src_ref=src, dst_ref=dst, send_sem=ss, recv_sem=rs,
            device_id={axis: lax.rem(target + size, size)}, device_id_type=MESH,
        )

    def sends(copy):
        _, idx, size, direction = copy[:4]
        return idx < size - 1 if direction == 0 else idx > 0

    def receives(copy):
        _, idx, size, direction = copy[:4]
        return idx > 0 if direction == 0 else idx < size - 1

    def start_all(copies):
        for copy in copies:
            if copy[2] > 1:
                pl.when(sends(copy))(lambda copy=copy: make(copy).start())

    def receive_all(copies):
        for copy in copies:
            if copy[2] > 1:
                pl.when(receives(copy))(lambda copy=copy: make(copy).wait_recv())

    def sent_all(copies):
        for copy in copies:
            if copy[2] > 1:
                pl.when(sends(copy))(lambda copy=copy: make(copy).wait_send())

    def span_copy(src, dst, ss, rs, partner):
        return pltpu.make_async_remote_copy(
            src_ref=src, dst_ref=dst, send_sem=ss, recv_sem=rs,
            device_id={"span": partner}, device_id_type=MESH,
        )

    def a2a_out(it, n):
        to = towards(*PARTNERS[n])
        return span_copy(
            send_a.at[it, to], recv_a.at[it, S], a2a_ss.at[it, n], a2a_rs.at[it, n], to
        )

    def a2a_back(it, n):
        to = back(*PARTNERS[n])
        return span_copy(
            send_r.at[it, to], recv_r.at[it, S], ret_ss.at[it, n], ret_rs.at[it, n], to
        )

    def ar_copies(k, stage):
        if stage == 0:
            return [
                span_copy(
                    ar_s.at[k, 0], ar_r.at[k, n], ar_ss.at[k, n], ar_rs.at[k, n], towards(*p)
                )
                for n, p in enumerate(PARTNERS)
            ]
        axis, idx, size = (("height", H, n_height), ("depth", D, n_depth))[stage - 1]
        first = 7 if stage == 1 else 10
        return [
            pltpu.make_async_remote_copy(
                src_ref=ar_s.at[k, stage], dst_ref=ar_r.at[k, first + d - 1],
                send_sem=ar_ss.at[k, first + d - 1], recv_sem=ar_rs.at[k, first + d - 1],
                device_id={axis: lax.rem(idx + d, size)}, device_id_type=MESH,
            )
            for d in range(1, size)
        ]

    def ar_begin(k, stage, value):
        ar_s[k, stage] = value
        for c in ar_copies(k, stage):
            c.start()

    def ar_end(k, stage, combine):
        copies = ar_copies(k, stage)
        for c in copies:
            c.wait_recv()
        first = (0, 7, 10)[stage]
        total = ar_s[k, stage]
        for n in range(len(copies)):
            total = combine(total, ar_r[k, first + n])
        return total

    def gather(it, row):
        def pack(i, _):
            for c in range(4):
                bx, by = c // 2, c % 2
                for j in range(0, 8, 2):
                    both = jnp.concatenate(
                        [row(8 * bx + i, 8 * by + j), row(8 * bx + i, 8 * by + j + 1)], axis=0
                    )
                    at = pl.multiple_of(i * 64, 64) + j * 8
                    lb[pl.ds(at, 16), c * 128 : (c + 1) * 128] = both.astype(BF16)
            return 0

        lax.fori_loop(0, 8, pack, 0)
        vs[...] = lax.dot_general(
            lb[...], sel[0:128, :], (((1,), (1,)), ((), ())), preferred_element_type=F32
        )

        def turn(g, _):
            start = pl.multiple_of(g * 128, 128)
            slots = block_transpose([vs[pl.ds(start + 8 * t, 8), :] for t in range(16)])
            for o in range(8):
                send_a[it, o, :, pl.ds(start, 128)] = jnp.concatenate(
                    [slots[2 * o], slots[2 * o + 1]], axis=0
                ).astype(BF16)
            return 0

        lax.fori_loop(0, 4, turn, 0)

    def own_product(it, src, lhs, out):
        for rank in range(2):
            result = jnp.dot(lhs[...], pre_v[src * 2 + rank], preferred_element_type=F32)
            out[rank * 8 : rank * 8 + 8, :] = result[rank * 8 : rank * 8 + 8, :]

    def precondition(it):
        if it == 0:
            pre_in[0].wait()
        own_product(it, S, send_a.at[it, S], recv_r.at[it, S])
        for n in range(7):
            if it == 0:
                pre_in[n + 1].wait()
            src = sources[n + 1]
            a2a_out(it, n).wait_recv()
            own_product(it, src, recv_a.at[it, src], send_r.at[it, src])
            a2a_back(it, n).start()

    def scatter(it):
        for n in range(7):
            a2a_back(it, n).wait_recv()

        def turn(g, _):
            start = pl.multiple_of(g * 128, 128)
            slots = [
                recv_r[it, s // 2, (s % 2) * 8 : (s % 2) * 8 + 8, pl.ds(start, 128)]
                for s in range(16)
            ]
            rows = block_transpose(slots)
            for t in range(0, 16, 2):
                both = jnp.concatenate([rows[t], rows[t + 1]], axis=0)
                high = both.astype(BF16)
                gbuf[pl.ds(start + 8 * t, 16), 0:128] = high
                gbuf[pl.ds(start + 8 * t, 16), 128:256] = (both - high.astype(F32)).astype(BF16)
            return 0

        lax.fori_loop(0, 4, turn, 0)

        def place(g, _):
            start = pl.multiple_of(g * 128, 128)
            chunk = gbuf[pl.ds(start, 128), :]
            cells = jnp.dot(chunk, sel[...], preferred_element_type=F32)
            faces = jnp.dot(chunk, ez[...], preferred_element_type=F32)
            packed = jnp.zeros((8, 128), F32)
            for t in range(16):
                ii, j = t // 8, t % 8
                for c in range(4):
                    bx, by = c // 2, c % 2
                    field[it, 1 + 8 * bx + 2 * g + ii, 1 + 8 * by + j] = cells[
                        t * 8 : t * 8 + 8, c * 128 : (c + 1) * 128
                    ]
                packed = jnp.where(lane // 8 == t, faces[t * 8 : t * 8 + 8, :], packed)
            hz_s[it, g] = packed
            return 0

        lax.fori_loop(0, 4, place, 0)

    def merge(right, left):
        return jnp.where(lane % 2 == 0, pltpu.roll(right, 127, 1), pltpu.roll(left, 1, 1))

    def small_faces(e):
        for side, y in ((0, 0), (1, 15)):
            sf_s[e, side] = ext[e, pl.ds(16 + y, 16, stride=16), :]

        def pack(x, packed):
            for h in range(2):
                n = x * 2 + h
                rows = ext[e, pl.ds(pl.multiple_of(x * 16 + 16, 8) + 8 * h, 8), :]
                packed = jnp.where(lane // 2 == n, pltpu.roll(rows, 2 * n + 1, 1), packed)
            return packed

        sf_s[e, 2, 0:8, :] = lax.fori_loop(0, 16, pack, jnp.zeros((8, 128), F32))

    def small_merge(e):
        sf_m[e] = merge(sf_r[e, 2, 8:16, :], sf_r[e, 2, 0:8, :])

    sub16 = lax.broadcasted_iota(jnp.int32, (16, 128), 0)
    lane16 = lax.broadcasted_iota(jnp.int32, (16, 128), 1)

    def small_block(e, x):
        return ext[e, pl.ds(pl.multiple_of(x * 16 + 16, 16), 16), :]

    def small_neighbours(e, x):
        mid = small_block(e, x)
        xp = ext[e, pl.ds(pl.multiple_of(x * 16 + 32, 16), 16), :]
        xm = ext[e, pl.ds(pl.multiple_of(x * 16, 16), 16), :]
        low = jnp.broadcast_to(sf_r[e, 0, pl.ds(x, 1), :], (16, 128))
        high = jnp.broadcast_to(sf_r[e, 1, pl.ds(x, 1), :], (16, 128))
        yp = jnp.where(sub16 == 15, high, pltpu.roll(mid, 15, 0))
        ym = jnp.where(sub16 == 0, low, pltpu.roll(mid, 1, 0))
        sides = jnp.concatenate(
            [pltpu.roll(sf_m[e], 127 - 2 * (2 * x + h), 1) for h in range(2)], axis=0
        )
        zp = jnp.where(lane16 == 127, sides, pltpu.roll(mid, 127, 1))
        zm = jnp.where(lane16 == 0, sides, pltpu.roll(mid, 1, 1))
        return xp, xm, yp, ym, zp, zm

    def small_sum(e, x):
        xp, xm, yp, ym, zp, zm = small_neighbours(e, x)
        return xp + xm + yp + ym + zp + zm

    def mask_block(x):
        bx = x // 8
        both = mrow[pl.ds(2 * bx, 2), :]
        return jnp.where(
            sub16 < 8,
            jnp.broadcast_to(both[0:1, :], (16, 128)),
            jnp.broadcast_to(both[1:2, :], (16, 128)),
        )

    def rows_of(x):
        return pl.ds(pl.multiple_of(x * 16, 16), 16)

    def clear_halos():
        zero_plane = jnp.zeros((16, 8, 128), F32)
        zero_face = jnp.zeros((16, 128), F32)

        def clear(cond, fn):
            pl.when(cond)(fn)

        def span_low():
            for it in range(2):
                field[it, 0, 1:17] = zero_plane
            for e in range(4):
                ext[e, 0:16, :] = zero_face

        def span_high():
            for it in range(2):
                field[it, 17, 1:17] = zero_plane
            for e in range(4):
                ext[e, 272:288, :] = zero_face

        def height_low():
            for it in range(2):
                field[it, 1:17, 0] = zero_plane
            for e in range(4):
                sf_r[e, 0] = zero_face

        def height_high():
            for it in range(2):
                field[it, 1:17, 17] = zero_plane
            for e in range(4):
                sf_r[e, 1] = zero_face

        def depth_low():
            for it in range(2):
                hz_r[it, 0] = jnp.zeros((4, 8, 128), F32)
            for e in range(4):
                sf_r[e, 2, 0:8, :] = jnp.zeros((8, 128), F32)

        def depth_high():
            for it in range(2):
                hz_r[it, 1] = jnp.zeros((4, 8, 128), F32)
            for e in range(4):
                sf_r[e, 2, 8:16, :] = jnp.zeros((8, 128), F32)

        clear(S == 0, span_low)
        clear(S == n_span - 1, span_high)
        clear(H == 0, height_low)
        clear(H == n_height - 1, height_high)
        clear(D == 0, depth_low)
        clear(D == n_depth - 1, depth_high)

    def setup_masked_stiffness():
        phase_in.wait()

        def body(x, _):
            p = small_block(1, x)
            stiff = void_stiffness + (1.0 - void_stiffness) * (p * p * p)
            ext[0, pl.ds(pl.multiple_of(x * 16 + 16, 16), 16), :] = mask_block(x) * stiff
            return 0

        lax.fori_loop(0, 16, body, 0)
        for e in range(2):
            small_faces(e)
            start_all(small_copies(e))

    def setup_coefficients():
        for e in range(2):
            receive_all(small_copies(e))
            small_merge(e)

        def body(x, _):
            p = small_block(1, x)
            stiff = void_stiffness + (1.0 - void_stiffness) * (p * p * p)
            m = mask_block(x)
            half = 0.5 * m
            total = m * spring_rate
            w = []
            for near in small_neighbours(0, x):
                one = half * (jnp.where(near > 0.0, stiff, 0.0) + near)
                total = total + one
                w.append(one)
            at = rows_of(x)
            dco[at, :] = total
            wx[pl.ds(pl.multiple_of(x * 16 + 16, 16), 16), :] = w[0]
            wx[at, :] = w[1]
            wyp[at, :] = w[2]
            wym[at, :] = w[3]
            wzl[at, :] = jnp.where(lane16 == 127, 0.0, w[4])
            wze[at, :] = jnp.where(lane16 == 127, w[4], jnp.where(lane16 == 0, w[5], 0.0))
            b = p / time_step - 0.5 * p * (1.0 - p) * (1.0 - 2.0 * p)
            base[at, :] = b
            ext[2, pl.ds(pl.multiple_of(x * 16 + 16, 16), 16), :] = inverse * (
                b + interface_weight * small_sum(1, x)
            )
            return 0

        lax.fori_loop(0, 16, body, 0)
        small_faces(2)
        start_all(small_copies(2))

    def setup_phase_part():
        receive_all(small_copies(2))
        small_merge(2)

        def body(x, _):
            at = rows_of(x)
            hpart[at, :] = inverse * (base[at, :] + interface_weight * small_sum(2, x))
            return 0

        lax.fori_loop(0, 16, body, 0)

    def load_row(x, y):
        return load_v[pl.ds(x * 16 + y, 8, stride=PITCH), :]

    def side_values(source, x, y):
        n = ((x % 2) * 8 + y % 8) * 4 + (x // 8) * 2 + y // 8
        return pltpu.roll(source, 127 - 2 * n, 1)

    def apply(it, x, y, hz):
        r = pl.ds(x * 16 + y, 1)
        v = field[it, x + 1, y + 1]
        wz = wzl[r, :]
        q = dco[r, :] * v
        q = q - wx[r, :] * field[it, x, y + 1]
        q = q - wx[pl.ds(x * 16 + 16 + y, 1), :] * field[it, x + 2, y + 1]
        q = q - wym[r, :] * field[it, x + 1, y]
        q = q - wyp[r, :] * field[it, x + 1, y + 2]
        q = q - wz * pltpu.roll(v, 127, 1) - pltpu.roll(wz * v, 1, 1)
        q = q - wze[r, :] * side_values(hz, x, y)
        return v, q

    def sums(*accumulated):
        packed = jnp.zeros((8, 128), F32)
        for n, a in enumerate(accumulated):
            packed = jnp.where(lane == n, jnp.sum(a, axis=1, keepdims=True), packed)
        return packed

    def receive_halos(it):
        receive_all(halo_copies(it))
        for g in range(4):
            hz_m[it, g] = merge(hz_r[it, 1, g], hz_r[it, 0, g])

    zero = jnp.zeros((8, 128), F32)
    add = lambda a, b: a + b

    for c in load_in:
        c.wait()
    gather(0, load_row)
    pl.semaphore_wait(barrier, 7 + (n_height - 1) + (n_depth - 1))
    for n in FAR_FIRST:
        a2a_out(0, n).start()
    clear_halos()
    setup_masked_stiffness()
    precondition(0)
    setup_coefficients()
    scatter(0)
    start_all(halo_copies(0))
    setup_phase_part()
    receive_halos(0)

    def first(x, carry):
        rz, zq = carry
        hz = hz_m[0, (x % 8) // 2]
        for y in range(16):
            v, q = apply(0, x, y, hz)
            image[x, y] = q
            rz = rz + load_row(x, y) * v
            zq = zq + v * q
        return rz, zq

    rz, zq = lax.fori_loop(0, 16, first, (zero, zero))
    ar_begin(0, 0, sums(rz, zq))
    gather(1, lambda x, y: image[x, y])
    for n in FAR_FIRST:
        a2a_out(1, n).start()
    ar_begin(0, 1, ar_end(0, 0, add))
    precondition(1)
    ar_begin(0, 2, ar_end(0, 1, add))
    scatter(1)
    start_all(halo_copies(1))
    total = ar_end(0, 2, add)
    rz1 = jnp.broadcast_to(total[:, 0:1], (8, 128))
    zq1 = jnp.broadcast_to(total[:, 1:2], (8, 128))
    alpha1 = rz1 / zq1
    receive_halos(1)

    def second(x, carry):
        rz, zaz, zq = carry
        hz = hz_m[1, (x % 8) // 2]
        for y in range(16):
            w, u = apply(1, x, y, hz)
            q1 = image[x, y]
            z2 = field[0, x + 1, y + 1] - alpha1 * w
            rz = rz + (load_row(x, y) - alpha1 * q1) * z2
            zaz = zaz + z2 * (q1 - alpha1 * u)
            zq = zq + z2 * q1
        return rz, zaz, zq

    ar_begin(1, 0, sums(*lax.fori_loop(0, 16, second, (zero, zero, zero))))
    ar_begin(1, 1, ar_end(1, 0, add))
    ar_begin(1, 2, ar_end(1, 1, add))
    total = ar_end(1, 2, add)
    rz2 = jnp.broadcast_to(total[:, 0:1], (8, 128))
    zaz = jnp.broadcast_to(total[:, 1:2], (8, 128))
    zq2 = jnp.broadcast_to(total[:, 2:3], (8, 128))
    beta = rz2 / rz1
    alpha2 = rz2 / (zaz + beta * (2.0 * zq2 + beta * zq1))
    on_z = alpha1 + alpha2 * (1.0 + beta)
    on_w = -alpha2 * alpha1

    def combine(x, y):
        value = on_z * field[0, x, y] + on_w * field[1, x, y]
        xfield[x, y] = value
        return value

    for x in (0, 17):
        for y in range(1, 17):
            combine(x, y)

    def form(x, _):
        combine(x + 1, 0)
        for y in range(16):
            dx[pl.ds(x * 16 + y, 8, stride=PITCH), :] = combine(x + 1, y + 1)
        combine(x + 1, 17)
        return 0

    lax.fori_loop(0, 16, form, 0)
    for g in range(4):
        hz_m[0, g] = on_z * hz_m[0, g] + on_w * hz_m[1, g]
    disp_out = [
        pltpu.make_async_copy(
            dx.at[pl.ds(l * PITCH, 256)], disp_hbm.at[pl.ds(l * 256, 256)], out_sem.at[l]
        )
        for l in range(8)
    ]
    for c in disp_out:
        c.start()

    def energy(x, peak):
        hz = hz_m[0, (x % 8) // 2]
        for y in range(16):
            r = pl.ds(x * 16 + y, 1)
            v = xfield[x + 1, y + 1]
            e = zero
            for w, near in (
                (wx[r, :], xfield[x, y + 1]),
                (wx[pl.ds(x * 16 + 16 + y, 1), :], xfield[x + 2, y + 1]),
                (wym[r, :], xfield[x + 1, y]),
                (wyp[r, :], xfield[x + 1, y + 2]),
                (wze[r, :], side_values(hz, x, y)),
            ):
                d = v - near
                e = e + jnp.where(w > 0.0, 1.0, 0.0) * (d * d)
            d = v - pltpu.roll(v, 127, 1)
            t = jnp.where(wzl[r, :] > 0.0, 1.0, 0.0) * (d * d)
            e = e + t + pltpu.roll(t, 1, 1)
            erow[r, :] = jnp.sum(e, axis=0, keepdims=True)
        at = rows_of(x)
        p = small_block(1, x)
        s = (-1.5 * (1.0 - void_stiffness)) * (p * p) * mask_block(x) * erow[at, :]
        sens[at, :] = s
        ext[3, pl.ds(pl.multiple_of(x * 16 + 16, 16), 16), :] = inverse * s
        return jnp.maximum(peak, jnp.maximum(-s[0:8, :], -s[8:16, :]))

    peak = lax.fori_loop(0, 16, energy, zero)
    ar_begin(2, 0, peak)
    small_faces(3)
    start_all(small_copies(3))
    sens_out = pltpu.make_async_copy(sens, sens_hbm, out_sem.at[8])
    sens_out.start()
    receive_all(small_copies(3))
    small_merge(3)
    ar_begin(2, 1, ar_end(2, 0, jnp.maximum))

    def slope(x, _):
        at = rows_of(x)
        erow[at, :] = small_block(3, x) + (interface_weight * inverse) * small_sum(3, x)
        return 0

    lax.fori_loop(0, 16, slope, 0)
    ar_begin(2, 2, ar_end(2, 1, jnp.maximum))
    peak = ar_end(2, 2, jnp.maximum)
    peak = jnp.max(jnp.max(peak, axis=1, keepdims=True), axis=0, keepdims=True)
    scale = jnp.broadcast_to(1.0 / (peak + epsilon_peak), (16, 128))

    def finish(x, _):
        at = rows_of(x)
        nxt[at, :] = hpart[at, :] - erow[at, :] * scale
        return 0

    lax.fori_loop(0, 16, finish, 0)
    next_out = pltpu.make_async_copy(nxt, next_hbm, out_sem.at[9])
    next_out.start()

    for it in range(2):
        for n in range(7):
            a2a_out(it, n).wait_send()
            a2a_back(it, n).wait_send()
        sent_all(halo_copies(it))
    for e in range(4):
        sent_all(small_copies(e))
    for k in range(3):
        for stage in range(3):
            for c in ar_copies(k, stage):
                c.wait_send()
    for c in disp_out:
        c.wait()
    sens_out.wait()
    next_out.wait()


def solution(mesh):
    sizes = tuple(mesh.shape[a] for a in AXES)
    dma = pltpu.SemaphoreType.DMA
    vmem = pltpu.VMEM

    def local(load, phase, void, owner, precond):
        any_space = pl.BlockSpec(memory_space=pl.ANY)
        disp, sens, nxt = pl.pallas_call(
            functools.partial(kernel, sizes),
            name="design_step",
            out_shape=(
                jax.ShapeDtypeStruct((2048, 128), F32),
                jax.ShapeDtypeStruct((256, 128), F32),
                jax.ShapeDtypeStruct((256, 128), F32),
            ),
            in_specs=[any_space] * 5,
            out_specs=(any_space,) * 3,
            scratch_shapes=[
                vmem((8 * PITCH, 128), F32),
                vmem((2, 2, 16), jnp.int32),
                vmem((2, 2, 16), jnp.int32),
                vmem((16, 512, 512), BF16),
                vmem((256, 512), BF16),
                vmem((256, 128), BF16),
                vmem((8, 128), F32),
                vmem((512, 512), BF16),
                vmem((512, 128), F32),
                vmem((512, 256), BF16),
                vmem((2, 8, 16, 512), BF16),
                vmem((2, 8, 16, 512), BF16),
                vmem((2, 8, 16, 512), F32),
                vmem((2, 8, 16, 512), F32),
                vmem((2, 18, 18, 8, 128), F32),
                vmem((16, 16, 8, 128), F32),
                vmem((2, 4, 8, 128), F32),
                vmem((2, 2, 4, 8, 128), F32),
                vmem((2, 4, 8, 128), F32),
                vmem((18, 18, 8, 128), F32),
                vmem((8 * PITCH, 128), F32),
                vmem((4, 288, 128), F32),
                vmem((4, 3, 16, 128), F32),
                vmem((4, 3, 16, 128), F32),
                vmem((4, 8, 128), F32),
                vmem((256, 128), F32),
                vmem((272, 128), F32),
                vmem((256, 128), F32),
                vmem((256, 128), F32),
                vmem((256, 128), F32),
                vmem((256, 128), F32),
                vmem((256, 128), F32),
                vmem((256, 128), F32),
                vmem((256, 128), F32),
                vmem((256, 128), F32),
                vmem((256, 128), F32),
                vmem((3, 3, 8, 128), F32),
                vmem((3, 13, 8, 128), F32),
                dma((11,)),
                dma((8,)),
                dma((10,)),
                dma((2, 7)),
                dma((2, 7)),
                dma((2, 7)),
                dma((2, 7)),
                dma((2, 6)),
                dma((2, 6)),
                dma((4, 6)),
                dma((4, 6)),
                dma((3, 13)),
                dma((3, 13)),
            ],
            compiler_params=pltpu.CompilerParams(
                collective_id=0, has_side_effects=True, vmem_limit_bytes=48 * 2**20
            ),
        )(load.reshape(2048, 128), phase.reshape(256, 128), void, owner, precond)
        return (
            disp.reshape(8, 16, 16, 128),
            sens.reshape(16, 16, 128),
            nxt.reshape(16, 16, 128),
        )

    return jax.shard_map(
        local,
        mesh=mesh,
        in_specs=(P(None, *AXES), P(*AXES), P(*AXES), P(*AXES), P(AXES, None, None)),
        out_specs=(P(None, *AXES), P(*AXES), P(*AXES)),
        check_vma=False,
    )
```

```python
import functools

import jax
import jax.numpy as jnp
from jax import lax
from jax.experimental import pallas as pl
from jax.experimental.pallas import tpu as pltpu
from jax.sharding import PartitionSpec as P

AXES = ("span", "height", "depth")
MESH = pl.DeviceIdType.MESH
F32 = jnp.float32
BF16 = jnp.bfloat16

void_stiffness = 0.001
spring_rate = 0.05
time_step = 0.5
interface_weight = 0.5
epsilon_peak = 1e-06
inverse = 1.0 / (1.0 / time_step + 6.0 * interface_weight)

PITCH = 264

PARTNERS = ((0, 1), (1, 0), (3, 0), (1, 1), (3, 1), (2, 0), (2, 1))
FAR_FIRST = (5, 6, 1, 2, 3, 4, 0)


def block_transpose(rows):
    lane_block = lax.broadcasted_iota(jnp.int32, (8, 128), 1) // 8
    rows = [pltpu.roll(r, 8 * t, 1) if t else r for t, r in enumerate(rows)]
    for bit in (1, 2, 4, 8):
        taken = (lane_block % (2 * bit)) >= bit
        rows = [jnp.where(taken, rows[(t + bit) % 16], rows[t]) for t in range(16)]
    out = []
    for s in range(16):
        r = rows[(16 - s) % 16]
        out.append(pltpu.roll(r, 128 - 8 * s, 1) if s else r)
    return out


def kernel(
    sizes,
    load_hbm, phase_hbm, void_hbm, owner_hbm, precond_hbm,
    dx, sens, nxt,
    load_v, void_v, owner_v, pre_v, sel, ez, mrow, lb, vs, gbuf,
    send_a0, send_a1, recv_a0, recv_a1, send_r, recv_r, field, image, quads, hz_s, hz_r, hz_m, wzp,
    ext, sf_s, sf_r, sf_m, dco, wx, wyp, wym, wzl, wze, base, hpart, slope, rate, ar_s, ar_r,
    in_sem, pre_sem, a2a_ss, a2a_rs, ret_ss, ret_rs, halo_ss, halo_rs,
    sf_ss, sf_rs, ar_ss, ar_rs, far_sem,
):
    n_span, n_height, n_depth = sizes
    send_a, recv_a = (send_a0, send_a1), (recv_a0, recv_a1)
    S, H, D = (lax.axis_index(a) for a in AXES)
    yy, core = S // 2, S % 2
    lane = lax.broadcasted_iota(jnp.int32, (8, 128), 1)

    def towards(dy, dc):
        return lax.rem(yy + dy, 4) * 2 + (1 - core if dc else core)

    def back(dy, dc):
        return lax.rem(yy + 4 - dy, 4) * 2 + (1 - core if dc else core)

    load_in = [
        pltpu.make_async_copy(
            load_hbm.at[pl.ds(l * 256, 256)], load_v.at[pl.ds(l * PITCH, 256)], in_sem.at[l]
        )
        for l in range(8)
    ]
    void_in = pltpu.make_async_copy(void_hbm, void_v, in_sem.at[8])
    owner_in = pltpu.make_async_copy(owner_hbm, owner_v, in_sem.at[9])
    phase_in = pltpu.make_async_copy(phase_hbm, ext.at[1, pl.ds(16, 256)], in_sem.at[10])
    void_in.start()
    owner_in.start()
    for c in load_in:
        c.start()
    phase_in.start()

    barrier = pltpu.get_barrier_semaphore()
    for dy, dc in PARTNERS:
        pl.semaphore_signal(barrier, 1, device_id={"span": towards(dy, dc)}, device_id_type=MESH)
    for d in range(1, n_height):
        pl.semaphore_signal(
            barrier, 1, device_id={"height": lax.rem(H + d, n_height)}, device_id_type=MESH
        )
    for d in range(1, n_depth):
        pl.semaphore_signal(
            barrier, 1, device_id={"depth": lax.rem(D + d, n_depth)}, device_id_type=MESH
        )

    sources = [S] + [back(dy, dc) for dy, dc in PARTNERS]
    pre_in = [
        pltpu.make_async_copy(
            precond_hbm.at[pl.ds(src * 2, 2)], pre_v.at[pl.ds(src * 2, 2)], pre_sem.at[n]
        )
        for n, src in enumerate(sources)
    ]
    for c in pre_in:
        c.start()

    void_in.wait()
    owner_in.wait()
    o_row = lax.broadcasted_iota(jnp.int32, (8, 16), 0)
    onehots = []
    for bx in range(2):
        own2, solid2 = owner_v[bx], 1 - void_v[bx]
        for by in range(2):
            own_row = jnp.broadcast_to(own2[by : by + 1, :], (8, 16))
            sol_row = jnp.broadcast_to(solid2[by : by + 1, :], (8, 16))
            onehots.append(jnp.where((own_row == o_row) & (sol_row == 1), 1.0, 0.0))
    onehot = jnp.concatenate(onehots, axis=0)
    b_row = lax.broadcasted_iota(jnp.int32, (16, 128), 0)
    b_lane = lax.broadcasted_iota(jnp.int32, (16, 128), 1) // 8
    spread = jnp.concatenate(
        [
            jnp.where(b_row == b_lane, 1.0, 0.0),
            jnp.where(b_row < b_lane, 1.0, 0.0),
            jnp.ones((16, 128), F32),
        ],
        axis=1,
    )
    counted = jnp.dot(onehot, spread, preferred_element_type=F32)
    o_col = lax.broadcasted_iota(jnp.int32, (8, 128), 0).astype(F32)
    row_id = lax.broadcasted_iota(jnp.int32, (128, 128), 0).astype(F32)
    lane_row = lax.broadcasted_iota(jnp.int32, (1, 128), 1)
    previous = jnp.zeros((8, 128), F32)
    edge = jnp.full((1, 128), -1.0, F32)
    for c in range(4):
        here = counted[c * 8 : c * 8 + 8, 0:128]
        before = counted[c * 8 : c * 8 + 8, 128:256] + previous
        previous = previous + counted[c * 8 : c * 8 + 8, 256:384]
        solid = jnp.sum(here, axis=0, keepdims=True)
        slot = jnp.sum(here * (2.0 * o_col + before), axis=0, keepdims=True)
        code = jnp.where(solid > 0.5, slot * 8.0 + (lane_row % 8).astype(F32), -1.0)
        mrow[c : c + 1, :] = solid
        picked = jnp.where(row_id == code, 1.0, 0.0).astype(BF16)
        sel[0:128, c * 128 : (c + 1) * 128] = picked
        sel[128:256, c * 128 : (c + 1) * 128] = picked
        edge = jnp.where(lane_row % 8 == 2 * c, jnp.broadcast_to(code[:, 127:128], (1, 128)), edge)
        edge = jnp.where(lane_row % 8 == 2 * c + 1, jnp.broadcast_to(code[:, 0:1], (1, 128)), edge)
    picked = jnp.where(row_id == edge, 1.0, 0.0).astype(BF16)
    ez[0:128, :] = picked
    ez[128:256, :] = picked

    def halo_copies(it):
        f = field.at[it]
        inner = pl.ds(1, 16)
        copies = []
        for n, (axis, idx, size, src, dst) in enumerate(
            (
                ("span", S, n_span, f.at[16, inner], f.at[0, inner]),
                ("span", S, n_span, f.at[1, inner], f.at[17, inner]),
                ("height", H, n_height, f.at[inner, 16], f.at[inner, 0]),
                ("height", H, n_height, f.at[inner, 1], f.at[inner, 17]),
                ("depth", D, n_depth, hz_s.at[it], hz_r.at[it, 0]),
                ("depth", D, n_depth, hz_s.at[it], hz_r.at[it, 1]),
            )
        ):
            copies.append((axis, idx, size, n % 2, src, dst, halo_ss.at[it, n], halo_rs.at[it, n]))
        return copies

    def small_copies(e):
        f = ext.at[e]
        copies = []
        for n, (axis, idx, size, src, dst) in enumerate(
            (
                ("span", S, n_span, f.at[pl.ds(256, 16)], f.at[pl.ds(0, 16)]),
                ("span", S, n_span, f.at[pl.ds(16, 16)], f.at[pl.ds(272, 16)]),
                ("height", H, n_height, sf_s.at[e, 1], sf_r.at[e, 0]),
                ("height", H, n_height, sf_s.at[e, 0], sf_r.at[e, 1]),
                ("depth", D, n_depth, sf_s.at[e, 2, pl.ds(0, 8)], sf_r.at[e, 2, pl.ds(0, 8)]),
                ("depth", D, n_depth, sf_s.at[e, 2, pl.ds(0, 8)], sf_r.at[e, 2, pl.ds(8, 8)]),
            )
        ):
            copies.append((axis, idx, size, n % 2, src, dst, sf_ss.at[e, n], sf_rs.at[e, n]))
        return copies

    def make(copy):
        axis, idx, size, direction, src, dst, ss, rs = copy
        target = idx + 1 if direction == 0 else idx - 1
        return pltpu.make_async_remote_copy(
            src_ref=src, dst_ref=dst, send_sem=ss, recv_sem=rs,
            device_id={axis: lax.rem(target + size, size)}, device_id_type=MESH,
        )

    def sends(copy):
        _, idx, size, direction = copy[:4]
        return idx < size - 1 if direction == 0 else idx > 0

    def receives(copy):
        _, idx, size, direction = copy[:4]
        return idx > 0 if direction == 0 else idx < size - 1

    def start_all(copies):
        for copy in copies:
            if copy[2] > 1:
                pl.when(sends(copy))(lambda copy=copy: make(copy).start())

    def receive_all(copies):
        for copy in copies:
            if copy[2] > 1:
                pl.when(receives(copy))(lambda copy=copy: make(copy).wait_recv())

    def sent_all(copies):
        for copy in copies:
            if copy[2] > 1:
                pl.when(sends(copy))(lambda copy=copy: make(copy).wait_send())

    def span_copy(src, dst, ss, rs, partner):
        return pltpu.make_async_remote_copy(
            src_ref=src, dst_ref=dst, send_sem=ss, recv_sem=rs,
            device_id={"span": partner}, device_id_type=MESH,
        )

    def a2a_out(it, n):
        to = towards(*PARTNERS[n])
        return span_copy(
            send_a[it].at[to], recv_a[it].at[S], a2a_ss.at[it, n], a2a_rs.at[it, n], to
        )

    def a2a_back(it, n):
        to = back(*PARTNERS[n])
        return span_copy(
            send_r.at[it, to], recv_r.at[it, S], ret_ss.at[it, n], ret_rs.at[it, n], to
        )

    plane = [(h, d) for h in range(n_height) for d in range(n_depth) if h or d]

    def ar_copies(k, stage):
        copies = []
        for n, p in enumerate(PARTNERS if stage == 0 else plane):
            at = n + 7 * stage
            if stage == 0:
                target = {"span": towards(*p)}
            else:
                target = {
                    "height": lax.rem(H + p[0], n_height),
                    "depth": lax.rem(D + p[1], n_depth),
                }
            copies.append(
                pltpu.make_async_remote_copy(
                    src_ref=ar_s.at[k, stage], dst_ref=ar_r.at[k, at],
                    send_sem=ar_ss.at[k, at], recv_sem=ar_rs.at[k, at],
                    device_id=target, device_id_type=MESH,
                )
            )
        return copies

    def ar_begin(k, stage, value):
        ar_s[k, stage] = value
        for c in reversed(ar_copies(k, stage)):
            c.start()

    def ar_end(k, stage, combine):
        copies = ar_copies(k, stage)
        for c in copies:
            c.wait_recv()
        total = ar_s[k, stage]
        for n in range(len(copies)):
            total = combine(total, ar_r[k, 7 * stage + n])
        return total

    def gather(it, row):
        def pack(i, _):
            for c in range(4):
                bx, by = c // 2, c % 2
                for j in range(0, 8, 2):
                    both = jnp.concatenate(
                        [row(8 * bx + i, 8 * by + j), row(8 * bx + i, 8 * by + j + 1)], axis=0
                    )
                    at = pl.multiple_of(i * 64, 64) + j * 8
                    high = both.astype(BF16)
                    lb[pl.ds(at, 16), c * 128 : (c + 1) * 128] = high
                    if it == 1:
                        low = (both - high.astype(F32)).astype(BF16)
                        lb[pl.ds(at, 16), 512 + c * 128 : 512 + (c + 1) * 128] = low
            return 0

        lax.fori_loop(0, 8, pack, 0)
        by_slot = (((1,), (1,)), ((), ()))
        chosen = lax.dot_general(
            lb[:, 0:512], sel[0:128, :], by_slot, preferred_element_type=F32
        )
        if it == 1:
            chosen = chosen + lax.dot_general(
                lb[:, 512:1024], sel[0:128, :], by_slot, preferred_element_type=F32
            )
        vs[...] = chosen

        def turn(g, _):
            start = pl.multiple_of(g * 128, 128)
            slots = block_transpose([vs[pl.ds(start + 8 * t, 8), :] for t in range(16)])
            for o in range(8):
                both = jnp.concatenate([slots[2 * o], slots[2 * o + 1]], axis=0)
                high = both.astype(BF16)
                send_a[it][o, 0:16, pl.ds(start, 128)] = high
                if it == 1:
                    low = (both - high.astype(F32)).astype(BF16)
                    send_a[it][o, 16:32, pl.ds(start, 128)] = low
            return 0

        lax.fori_loop(0, 4, turn, 0)

    def own_product(it, src, lhs, out):
        for rank in range(2):
            result = jnp.dot(lhs[...], pre_v[src * 2 + rank], preferred_element_type=F32)
            part = result[rank * 8 : rank * 8 + 8, :]
            if it == 1:
                part = part + result[16 + rank * 8 : 24 + rank * 8, :]
            out[rank * 8 : rank * 8 + 8, :] = part

    def precondition(it):
        if it == 0:
            pre_in[0].wait()
        own_product(it, S, send_a[it].at[S], recv_r.at[it, S])
        for n in range(7):
            if it == 0:
                pre_in[n + 1].wait()
            src = sources[n + 1]
            a2a_out(it, n).wait_recv()
            own_product(it, src, recv_a[it].at[src], send_r.at[it, src])
            a2a_back(it, n).start()

    def scatter(it):
        for n in range(7):
            a2a_back(it, n).wait_recv()

        def turn(g, _):
            start = pl.multiple_of(g * 128, 128)
            slots = [
                recv_r[it, s // 2, (s % 2) * 8 : (s % 2) * 8 + 8, pl.ds(start, 128)]
                for s in range(16)
            ]
            rows = block_transpose(slots)
            for t in range(0, 16, 2):
                both = jnp.concatenate([rows[t], rows[t + 1]], axis=0)
                high = both.astype(BF16)
                gbuf[pl.ds(start + 8 * t, 16), 0:128] = high
                gbuf[pl.ds(start + 8 * t, 16), 128:256] = (both - high.astype(F32)).astype(BF16)
            return 0

        lax.fori_loop(0, 4, turn, 0)

        def place(g, _):
            start = pl.multiple_of(g * 128, 128)
            chunk = gbuf[pl.ds(start, 128), :]
            cells = jnp.dot(chunk, sel[...], preferred_element_type=F32)
            faces = jnp.dot(chunk, ez[...], preferred_element_type=F32)
            packed = jnp.zeros((8, 128), F32)
            for t in range(16):
                ii, j = t // 8, t % 8
                for c in range(4):
                    bx, by = c // 2, c % 2
                    field[it, 1 + 8 * bx + 2 * g + ii, 1 + 8 * by + j] = cells[
                        t * 8 : t * 8 + 8, c * 128 : (c + 1) * 128
                    ]
                packed = jnp.where(lane // 8 == t, faces[t * 8 : t * 8 + 8, :], packed)
            hz_s[it, g] = packed
            return 0

        lax.fori_loop(0, 4, place, 0)

    def merge(right, left):
        return jnp.where(lane % 2 == 0, pltpu.roll(right, 127, 1), pltpu.roll(left, 1, 1))

    def unrolled(count, step, body):
        def several(g, _):
            for k in range(step):
                body(g * step + k, 0)
            return 0

        lax.fori_loop(0, count // step, several, 0)

    def small_faces(e):
        for side, y in ((0, 0), (1, 15)):
            sf_s[e, side] = ext[e, pl.ds(16 + y, 16, stride=16), :]
        parts = [jnp.zeros((8, 128), F32)] * 4
        for n in range(32):
            rows = pltpu.roll(ext[e, 16 + 8 * n : 24 + 8 * n, :], 2 * n + 1, 1)
            parts[n % 4] = jnp.where(lane // 2 == n, rows, parts[n % 4])
        sf_s[e, 2, 0:8, :] = (parts[0] + parts[1]) + (parts[2] + parts[3])

    def small_merge(e):
        sf_m[e] = merge(sf_r[e, 2, 8:16, :], sf_r[e, 2, 0:8, :])

    sub16 = lax.broadcasted_iota(jnp.int32, (16, 128), 0)
    lane16 = lax.broadcasted_iota(jnp.int32, (16, 128), 1)

    def small_block(e, x):
        return ext[e, pl.ds(pl.multiple_of(x * 16 + 16, 16), 16), :]

    def small_neighbours(e, x):
        mid = small_block(e, x)
        xp = ext[e, pl.ds(pl.multiple_of(x * 16 + 32, 16), 16), :]
        xm = ext[e, pl.ds(pl.multiple_of(x * 16, 16), 16), :]
        low = jnp.broadcast_to(sf_r[e, 0, pl.ds(x, 1), :], (16, 128))
        high = jnp.broadcast_to(sf_r[e, 1, pl.ds(x, 1), :], (16, 128))
        yp = jnp.where(sub16 == 15, high, pltpu.roll(mid, 15, 0))
        ym = jnp.where(sub16 == 0, low, pltpu.roll(mid, 1, 0))
        sides = jnp.concatenate(
            [pltpu.roll(sf_m[e], 127 - 2 * (2 * x + h), 1) for h in range(2)], axis=0
        )
        zp = jnp.where(lane16 == 127, sides, pltpu.roll(mid, 127, 1))
        zm = jnp.where(lane16 == 0, sides, pltpu.roll(mid, 1, 1))
        return xp, xm, yp, ym, zp, zm

    def small_sum(e, x):
        xp, xm, yp, ym, zp, zm = small_neighbours(e, x)
        return xp + xm + yp + ym + zp + zm

    def mask_block(x):
        bx = x // 8
        both = mrow[pl.ds(2 * bx, 2), :]
        return jnp.where(
            sub16 < 8,
            jnp.broadcast_to(both[0:1, :], (16, 128)),
            jnp.broadcast_to(both[1:2, :], (16, 128)),
        )

    def rows_of(x):
        return pl.ds(pl.multiple_of(x * 16, 16), 16)

    def clear_halos():
        zero_plane = jnp.zeros((16, 8, 128), F32)
        zero_face = jnp.zeros((16, 128), F32)

        def clear(cond, fn):
            pl.when(cond)(fn)

        def span_low():
            for it in range(2):
                field[it, 0, 1:17] = zero_plane
            for e in range(4):
                ext[e, 0:16, :] = zero_face

        def span_high():
            for it in range(2):
                field[it, 17, 1:17] = zero_plane
            for e in range(4):
                ext[e, 272:288, :] = zero_face

        def height_low():
            for it in range(2):
                field[it, 1:17, 0] = zero_plane
            for e in range(4):
                sf_r[e, 0] = zero_face

        def height_high():
            for it in range(2):
                field[it, 1:17, 17] = zero_plane
            for e in range(4):
                sf_r[e, 1] = zero_face

        def depth_low():
            for it in range(2):
                hz_r[it, 0] = jnp.zeros((4, 8, 128), F32)
            for e in range(4):
                sf_r[e, 2, 0:8, :] = jnp.zeros((8, 128), F32)

        def depth_high():
            for it in range(2):
                hz_r[it, 1] = jnp.zeros((4, 8, 128), F32)
            for e in range(4):
                sf_r[e, 2, 8:16, :] = jnp.zeros((8, 128), F32)

        clear(S == 0, span_low)
        clear(S == n_span - 1, span_high)
        clear(H == 0, height_low)
        clear(H == n_height - 1, height_high)
        clear(D == 0, depth_low)
        clear(D == n_depth - 1, depth_high)

    def setup_masked_stiffness():
        phase_in.wait()

        def body(x, _):
            p = small_block(1, x)
            stiff = void_stiffness + (1.0 - void_stiffness) * (p * p * p)
            m = mask_block(x)
            ext[0, pl.ds(pl.multiple_of(x * 16 + 16, 16), 16), :] = m * stiff
            rate[rows_of(x), :] = (-1.5 * (1.0 - void_stiffness)) * (p * p) * m

        unrolled(16, 4, body)
        for e in range(2):
            small_faces(e)
            start_all(small_copies(e))

    def setup_coefficients():
        for e in range(2):
            receive_all(small_copies(e))
            small_merge(e)

        def body(x, _):
            p = small_block(1, x)
            stiff = void_stiffness + (1.0 - void_stiffness) * (p * p * p)
            m = mask_block(x)
            half = 0.5 * m
            total = m * spring_rate
            w = []
            for near in small_neighbours(0, x):
                one = half * (jnp.where(near > 0.0, stiff, 0.0) + near)
                total = total + one
                w.append(one)
            at = rows_of(x)
            dco[at, :] = total
            wx[pl.ds(pl.multiple_of(x * 16 + 16, 16), 16), :] = w[0]
            wx[at, :] = w[1]
            wyp[at, :] = w[2]
            wym[at, :] = w[3]
            wzl[at, :] = jnp.where(lane16 == 127, 0.0, w[4])
            wze[at, :] = jnp.where(lane16 == 127, w[4], jnp.where(lane16 == 0, w[5], 0.0))
            b = p / time_step - 0.5 * p * (1.0 - p) * (1.0 - 2.0 * p)
            base[at, :] = b
            ext[2, pl.ds(pl.multiple_of(x * 16 + 16, 16), 16), :] = inverse * (
                b + interface_weight * small_sum(1, x)
            )

        unrolled(16, 4, body)
        small_faces(2)
        start_all(small_copies(2))

    def setup_phase_part():
        receive_all(small_copies(2))
        small_merge(2)

        def body(x, _):
            at = rows_of(x)
            hpart[at, :] = inverse * (base[at, :] + interface_weight * small_sum(2, x))

        unrolled(16, 4, body)

    def load_row(x, y):
        return load_v[pl.ds(x * 16 + y, 8, stride=PITCH), :]

    def side_values(source, x, y):
        n = ((x % 2) * 8 + y % 8) * 4 + (x // 8) * 2 + y // 8
        return pltpu.roll(source, 127 - 2 * n, 1)

    def local(it, x, y, low, high):
        r = pl.ds(x * 16 + y, 1)
        v = field[it, x + 1, y + 1]
        wz = wzl[r, :]
        q = dco[r, :] * v
        if low:
            q = q - wx[r, :] * field[it, x, y + 1]
        if high:
            q = q - wx[pl.ds(x * 16 + 16 + y, 1), :] * field[it, x + 2, y + 1]
        if y > 0:
            q = q - wym[r, :] * field[it, x + 1, y]
        if y < 15:
            q = q - wyp[r, :] * field[it, x + 1, y + 2]
        return v, q - wz * pltpu.roll(v, 127, 1) - pltpu.roll(wz * v, 1, 1)

    def over_planes(body, carry):
        carry = body(0, carry, False, True)
        carry = lax.fori_loop(1, 15, lambda x, c: body(x, c, True, True), carry)
        return body(15, carry, True, False)

    lane_row8 = jnp.broadcast_to(lane_row, (8, 128))
    sub8 = lax.broadcasted_iota(jnp.int32, (8, 128), 0)

    def as_row(*accumulated):
        packed = jnp.zeros((8, 128), F32)
        for n, a in enumerate(accumulated):
            packed = jnp.where(lane_row8 == 8 * n + sub8, jnp.sum(a, axis=1, keepdims=True), packed)
        return jnp.sum(packed, axis=0, keepdims=True)

    def from_row(row, n):
        own = jnp.where(lane_row8 == 8 * n + sub8, jnp.broadcast_to(row, (8, 128)), 0.0)
        return jnp.broadcast_to(jnp.sum(own, axis=1, keepdims=True), (8, 128))

    def receive_halos(it):
        receive_all(halo_copies(it))
        for g in range(4):
            hz_m[it, g] = merge(hz_r[it, 1, g], hz_r[it, 0, g])

    def pack_edge_weights():
        def body(g, _):
            packed = [jnp.zeros((8, 128), F32)] * 4
            for ii in range(2):
                for c in range(4):
                    x = 8 * (c // 2) + 2 * g + ii
                    for j in range(8):
                        n = (ii * 8 + j) * 4 + c
                        row = wze[pl.ds(x * 16 + 8 * (c % 2) + j, 1), :]
                        row = pltpu.roll(jnp.broadcast_to(row, (8, 128)), 2 * n + 1, 1)
                        packed[c] = jnp.where(lane // 2 == n, row, packed[c])
            wzp[g] = (packed[0] + packed[1]) + (packed[2] + packed[3])
            return 0

        lax.fori_loop(0, 4, body, 0)

    def load_sums(rows):
        first = sub8 < 4
        out = []
        for y in range(4):
            a, b = rows[y], rows[y + 4]
            out.append(jnp.where(first, a, b) + pltpu.roll(jnp.where(first, b, a), 4, 0))
        rows = out
        for half in (2, 1):
            first = (sub8 % (2 * half)) < half
            out = []
            for y in range(half):
                a, b = rows[y], rows[y + half]
                other = jnp.where(first, b, a)
                moved = jnp.where(
                    first, pltpu.roll(other, 8 - half, 0), pltpu.roll(other, half, 0)
                )
                out.append(jnp.where(first, a, b) + moved)
            rows = out
        return rows[0]

    zero = jnp.zeros((8, 128), F32)
    add = lambda a, b: a + b

    for c in load_in:
        c.wait()
    gather(0, load_row)
    pl.semaphore_wait(barrier, 7 + (n_height - 1) + (n_depth - 1))
    for n in FAR_FIRST:
        a2a_out(0, n).start()
    for d in range(1, n_height):
        pl.semaphore_signal(
            far_sem, 1, device_id={"height": lax.rem(H + d, n_height)}, device_id_type=MESH
        )
    clear_halos()
    setup_masked_stiffness()
    precondition(0)
    setup_coefficients()
    scatter(0)
    start_all(halo_copies(0))

    def local_first(x, carry, low, high):
        for y in range(16):
            image[x, y] = local(0, x, y, low, high)[1]
        return carry

    over_planes(local_first, 0)
    receive_halos(0)
    for y in range(16):
        image[0, y] = image[0, y] - wx[y : y + 1, :] * field[0, 0, y + 1]
        image[15, y] = image[15, y] - wx[256 + y : 257 + y, :] * field[0, 17, y + 1]

    def image_row(x, y):
        r = pl.ds(x * 16 + y, 1)
        q = image[x, y] - wze[r, :] * side_values(hz_m[0, (x % 8) // 2], x, y)
        if y == 0:
            q = q - wym[r, :] * field[0, x + 1, 0]
        if y == 15:
            q = q - wyp[r, :] * field[0, x + 1, 17]
        image[x, y] = q
        return q

    gather(1, image_row)
    for n in FAR_FIRST:
        a2a_out(1, n).start()

    def first_sums(x, carry):
        rz, zq = carry
        for y in range(16):
            v = field[0, x + 1, y + 1]
            rz = rz + load_row(x, y) * v
            zq = zq + image[x, y] * v
        return rz, zq

    ar_begin(0, 0, as_row(*lax.fori_loop(0, 16, first_sums, (zero, zero))))
    setup_phase_part()
    pack_edge_weights()
    precondition(1)
    if n_height > 1:
        pl.semaphore_wait(far_sem, n_height - 1)
    ar_begin(0, 1, ar_end(0, 0, add))
    scatter(1)
    start_all(halo_copies(1))
    total = ar_end(0, 1, add)
    rz1 = from_row(total, 0)
    zq1 = from_row(total, 1)
    alpha1 = rz1 / zq1

    def local_second(x, carry, low, high):
        rz, zaz, zq = carry
        for y in range(16):
            w, u = local(1, x, y, low, high)
            q1 = image[x, y]
            z2 = field[0, x + 1, y + 1] - alpha1 * w
            rz = rz + (load_row(x, y) - alpha1 * q1) * z2
            zaz = zaz + z2 * (q1 - alpha1 * u)
            zq = zq + z2 * q1
        return rz, zaz, zq

    rz, zaz, zq = over_planes(local_second, (zero, zero, zero))
    receive_halos(1)

    def second_direction(x, y):
        return field[0, x + 1, y + 1] - alpha1 * field[1, x + 1, y + 1]

    outer = zero
    for y in range(16):
        outer = outer + second_direction(0, y) * (wx[y : y + 1, :] * field[1, 0, y + 1])
        outer = outer + second_direction(15, y) * (wx[256 + y : 257 + y, :] * field[1, 17, y + 1])
        outer = outer + second_direction(y, 0) * (wym[16 * y : 16 * y + 1, :] * field[1, y + 1, 0])
        outer = outer + second_direction(y, 15) * (
            wyp[16 * y + 15 : 16 * y + 16, :] * field[1, y + 1, 17]
        )
    for g in range(4):
        outer = outer + (hz_s[0, g] - alpha1 * hz_s[1, g]) * (wzp[g] * hz_m[1, g])
    ar_begin(1, 0, as_row(rz, zaz + alpha1 * outer, zq))

    def quadratic(x, _):
        hz0 = hz_m[0, (x % 8) // 2]
        hz1 = hz_m[1, (x % 8) // 2]
        for y in range(16):
            r = pl.ds(x * 16 + y, 1)
            z, w = field[0, x + 1, y + 1], field[1, x + 1, y + 1]
            zz = zw = ww = zero
            for weight, near_z, near_w in (
                (wx[r, :], field[0, x, y + 1], field[1, x, y + 1]),
                (wx[pl.ds(x * 16 + 16 + y, 1), :], field[0, x + 2, y + 1], field[1, x + 2, y + 1]),
                (wym[r, :], field[0, x + 1, y], field[1, x + 1, y]),
                (wyp[r, :], field[0, x + 1, y + 2], field[1, x + 1, y + 2]),
                (wze[r, :], side_values(hz0, x, y), side_values(hz1, x, y)),
            ):
                solid = weight > 0.0
                dz = jnp.where(solid, z - near_z, 0.0)
                dw = jnp.where(solid, w - near_w, 0.0)
                zz, zw, ww = zz + dz * dz, zw + dz * dw, ww + dw * dw
            solid = wzl[r, :] > 0.0
            dz = jnp.where(solid, z - pltpu.roll(z, 127, 1), 0.0)
            dw = jnp.where(solid, w - pltpu.roll(w, 127, 1), 0.0)
            uz, uw = pltpu.roll(dz, 1, 1), pltpu.roll(dw, 1, 1)
            quads[0, x, y] = zz + dz * dz + uz * uz
            quads[1, x, y] = zw + dz * dw + uz * uw
            quads[2, x, y] = ww + dw * dw + uw * uw
        return 0

    lax.fori_loop(0, 8, quadratic, 0)
    ar_begin(1, 1, ar_end(1, 0, add))
    lax.fori_loop(8, 16, quadratic, 0)
    total = ar_end(1, 1, add)
    rz2 = from_row(total, 0)
    zaz = from_row(total, 1)
    zq2 = from_row(total, 2)
    beta = rz2 / rz1
    alpha2 = rz2 / (zaz + beta * (2.0 * zq2 + beta * zq1))
    on_z = alpha1 + alpha2 * (1.0 + beta)
    on_w = -alpha2 * alpha1
    on_zz, on_zw, on_ww = on_z * on_z, 2.0 * on_z * on_w, on_w * on_w

    def sensitivities(x, peak):
        for h in range(2):
            energy = load_sums(
                [
                    on_zz * quads[0, x, 8 * h + y]
                    + on_zw * quads[1, x, 8 * h + y]
                    + on_ww * quads[2, x, 8 * h + y]
                    for y in range(8)
                ]
            )
            at = pl.multiple_of(x * 16, 16) + 8 * h
            s = rate[pl.ds(at, 8), :] * energy
            sens[pl.ds(at, 8), :] = s
            ext[3, pl.ds(at + 16, 8), :] = inverse * s
            peak = jnp.maximum(peak, -s)
        return peak

    peak = lax.fori_loop(0, 16, sensitivities, zero)
    ar_begin(2, 0, jnp.max(peak, axis=0, keepdims=True))
    small_faces(3)
    start_all(small_copies(3))

    def form(x, _):
        for y in range(16):
            dx[pl.ds(x * 16 + y, 8, stride=PITCH), :] = (
                on_z * field[0, x + 1, y + 1] + on_w * field[1, x + 1, y + 1]
            )
        return 0

    lax.fori_loop(0, 16, form, 0)
    ar_begin(2, 1, ar_end(2, 0, jnp.maximum))
    receive_all(small_copies(3))
    small_merge(3)

    def slopes(x, _):
        slope[rows_of(x), :] = small_block(3, x) + (interface_weight * inverse) * small_sum(3, x)

    unrolled(16, 4, slopes)
    peak = jnp.max(ar_end(2, 1, jnp.maximum), axis=1, keepdims=True)
    scale = jnp.broadcast_to(1.0 / (peak + epsilon_peak), (8, 128))
    for n in range(32):
        at = slice(8 * n, 8 * n + 8)
        nxt[at, :] = hpart[at, :] - slope[at, :] * scale

    for it in range(2):
        for n in range(7):
            a2a_out(it, n).wait_send()
            a2a_back(it, n).wait_send()
        sent_all(halo_copies(it))
    for e in range(4):
        sent_all(small_copies(e))
    for k in range(3):
        for stage in range(2):
            for c in ar_copies(k, stage):
                c.wait_send()


def deliver(dx, sens, nxt, disp_hbm, sens_hbm, next_hbm, sem):
    copies = [
        pltpu.make_async_copy(
            dx.at[pl.ds(l * PITCH, 256)], disp_hbm.at[pl.ds(l * 256, 256)], sem.at[l]
        )
        for l in range(8)
    ]
    copies.append(pltpu.make_async_copy(sens, sens_hbm, sem.at[8]))
    copies.append(pltpu.make_async_copy(nxt, next_hbm, sem.at[9]))
    for c in copies:
        c.start()
    for c in copies:
        c.wait()


def solution(mesh):
    sizes = tuple(mesh.shape[a] for a in AXES)
    dma = pltpu.SemaphoreType.DMA
    vmem = pltpu.VMEM

    def local(load, phase, void, owner, precond):
        vmem_space = pl.BlockSpec(memory_space=pltpu.VMEM)
        hbm_space = pl.BlockSpec(memory_space=pltpu.HBM)
        results = pl.pallas_call(
            functools.partial(kernel, sizes),
            name="design_step",
            out_shape=(
                jax.ShapeDtypeStruct((8 * PITCH, 128), F32),
                jax.ShapeDtypeStruct((256, 128), F32),
                jax.ShapeDtypeStruct((256, 128), F32),
            ),
            in_specs=[hbm_space] * 5,
            out_specs=(vmem_space,) * 3,
            scratch_shapes=[
                vmem((8 * PITCH, 128), F32),
                vmem((2, 2, 16), jnp.int32),
                vmem((2, 2, 16), jnp.int32),
                vmem((16, 512, 512), BF16),
                vmem((256, 512), BF16),
                vmem((256, 128), BF16),
                vmem((8, 128), F32),
                vmem((512, 1024), BF16),
                vmem((512, 128), F32),
                vmem((512, 256), BF16),
                vmem((8, 16, 512), BF16),
                vmem((8, 32, 512), BF16),
                vmem((8, 16, 512), BF16),
                vmem((8, 32, 512), BF16),
                vmem((2, 8, 16, 512), F32),
                vmem((2, 8, 16, 512), F32),
                vmem((2, 18, 18, 8, 128), F32),
                vmem((16, 16, 8, 128), F32),
                vmem((3, 16, 16, 8, 128), F32),
                vmem((2, 4, 8, 128), F32),
                vmem((2, 2, 4, 8, 128), F32),
                vmem((2, 4, 8, 128), F32),
                vmem((4, 8, 128), F32),
                vmem((4, 288, 128), F32),
                vmem((4, 3, 16, 128), F32),
                vmem((4, 3, 16, 128), F32),
                vmem((4, 8, 128), F32),
                vmem((256, 128), F32),
                vmem((272, 128), F32),
                vmem((256, 128), F32),
                vmem((256, 128), F32),
                vmem((256, 128), F32),
                vmem((256, 128), F32),
                vmem((256, 128), F32),
                vmem((256, 128), F32),
                vmem((256, 128), F32),
                vmem((256, 128), F32),
                vmem((3, 2, 1, 128), F32),
                vmem((3, 22, 1, 128), F32),
                dma((11,)),
                dma((8,)),
                dma((2, 7)),
                dma((2, 7)),
                dma((2, 7)),
                dma((2, 7)),
                dma((2, 6)),
                dma((2, 6)),
                dma((4, 6)),
                dma((4, 6)),
                dma((3, 22)),
                dma((3, 22)),
                pltpu.SemaphoreType.REGULAR,
            ],
            compiler_params=pltpu.CompilerParams(
                collective_id=0, has_side_effects=True, vmem_limit_bytes=48 * 2**20
            ),
        )(*(
            pltpu.with_memory_space_constraint(a, pltpu.HBM)
            for a in (load.reshape(2048, 128), phase.reshape(256, 128), void, owner, precond)
        ))
        disp, sens, nxt = pl.pallas_call(
            deliver,
            name="deliver",
            out_shape=(
                jax.ShapeDtypeStruct((2048, 128), F32),
                jax.ShapeDtypeStruct((256, 128), F32),
                jax.ShapeDtypeStruct((256, 128), F32),
            ),
            in_specs=[pl.BlockSpec(memory_space=pl.ANY)] * 3,
            out_specs=(hbm_space,) * 3,
            scratch_shapes=[dma((10,))],
            compiler_params=pltpu.CompilerParams(vmem_limit_bytes=2**20),
        )(*results)
        return (
            disp.reshape(8, 16, 16, 128),
            sens.reshape(16, 16, 128),
            nxt.reshape(16, 16, 128),
        )

    return jax.shard_map(
        local,
        mesh=mesh,
        in_specs=(P(None, *AXES), P(*AXES), P(*AXES), P(*AXES), P(AXES, None, None)),
        out_specs=(P(None, *AXES), P(*AXES), P(*AXES)),
        check_vma=False,
    )
```

```python
import functools

import jax
import jax.numpy as jnp
from jax import lax
from jax.experimental import pallas as pl
from jax.experimental.pallas import tpu as pltpu
from jax.sharding import PartitionSpec as P

AXES = ("span", "height", "depth")
MESH = pl.DeviceIdType.MESH
F32 = jnp.float32
BF16 = jnp.bfloat16

void_stiffness = 0.001
spring_rate = 0.05
time_step = 0.5
interface_weight = 0.5
epsilon_peak = 1e-06
inverse = 1.0 / (1.0 / time_step + 6.0 * interface_weight)

PITCH = 264

PARTNERS = ((0, 1), (1, 0), (3, 0), (1, 1), (3, 1), (2, 0), (2, 1))


def block_transpose(rows):
    lane_block = lax.broadcasted_iota(jnp.int32, (8, 128), 1) // 8
    rows = [pltpu.roll(r, 8 * t, 1) if t else r for t, r in enumerate(rows)]
    for bit in (1, 2, 4, 8):
        taken = (lane_block % (2 * bit)) >= bit
        rows = [jnp.where(taken, rows[(t + bit) % 16], rows[t]) for t in range(16)]
    out = []
    for s in range(16):
        r = rows[(16 - s) % 16]
        out.append(pltpu.roll(r, 128 - 8 * s, 1) if s else r)
    return out


def kernel(
    sizes,
    load_hbm, phase_hbm, void_hbm, owner_hbm, precond_hbm,
    dx, sens, nxt,
    load_v, void_v, owner_v, pre_v, sel, ez, mrow, lb, gbuf,
    send_a0, send_a1, recv_a0, recv_a1, send_r, recv_r, field, image, quads, hz_s, hz_r, hz_m, wzp,
    ext, sf_s, sf_r, sf_m, dco, wx, wyp, wym, wzl, wze, base, hpart, slope, rate, ar_s, ar_r,
    in_sem, pre_sem, a2a_ss, a2a_rs, ret_ss, ret_rs, halo_ss, halo_rs,
    sf_ss, sf_rs, ar_ss, ar_rs, far_sem,
):
    n_span, n_height, n_depth = sizes
    send_a, recv_a = (send_a0, send_a1), (recv_a0, recv_a1)
    S, H, D = (lax.axis_index(a) for a in AXES)
    yy, core = S // 2, S % 2
    lane = lax.broadcasted_iota(jnp.int32, (8, 128), 1)

    def towards(dy, dc):
        return lax.rem(yy + dy, 4) * 2 + (1 - core if dc else core)

    def back(dy, dc):
        return lax.rem(yy + 4 - dy, 4) * 2 + (1 - core if dc else core)

    load_in = [
        pltpu.make_async_copy(
            load_hbm.at[pl.ds(l * 256, 256)], load_v.at[pl.ds(l * PITCH, 256)], in_sem.at[l]
        )
        for l in range(8)
    ]
    void_in = pltpu.make_async_copy(void_hbm, void_v, in_sem.at[8])
    owner_in = pltpu.make_async_copy(owner_hbm, owner_v, in_sem.at[9])
    phase_in = pltpu.make_async_copy(phase_hbm, ext.at[1, pl.ds(16, 256)], in_sem.at[10])
    void_in.start()
    owner_in.start()
    for c in load_in:
        c.start()
    phase_in.start()

    barrier = pltpu.get_barrier_semaphore()
    for dy, dc in PARTNERS:
        pl.semaphore_signal(barrier, 1, device_id={"span": towards(dy, dc)}, device_id_type=MESH)
    for d in range(1, n_height):
        pl.semaphore_signal(
            barrier, 1, device_id={"height": lax.rem(H + d, n_height)}, device_id_type=MESH
        )
    for d in range(1, n_depth):
        pl.semaphore_signal(
            barrier, 1, device_id={"depth": lax.rem(D + d, n_depth)}, device_id_type=MESH
        )

    sources = [S] + [back(dy, dc) for dy, dc in PARTNERS]
    pre_in = [
        pltpu.make_async_copy(
            precond_hbm.at[pl.ds(src * 2, 2)], pre_v.at[pl.ds(src * 2, 2)], pre_sem.at[n]
        )
        for n, src in enumerate(sources)
    ]
    for c in pre_in:
        c.start()

    lane_row = lax.broadcasted_iota(jnp.int32, (1, 128), 1)

    def plan():
        void_in.wait()
        owner_in.wait()
        o_row = lax.broadcasted_iota(jnp.int32, (8, 16), 0)
        onehots = []
        for bx in range(2):
            own2, solid2 = owner_v[bx], 1 - void_v[bx]
            for by in range(2):
                own_row = jnp.broadcast_to(own2[by : by + 1, :], (8, 16))
                sol_row = jnp.broadcast_to(solid2[by : by + 1, :], (8, 16))
                onehots.append(jnp.where((own_row == o_row) & (sol_row == 1), 1.0, 0.0))
        onehot = jnp.concatenate(onehots, axis=0)
        b_row = lax.broadcasted_iota(jnp.int32, (16, 128), 0)
        b_lane = lax.broadcasted_iota(jnp.int32, (16, 128), 1) // 8
        spread = jnp.concatenate(
            [
                jnp.where(b_row == b_lane, 1.0, 0.0),
                jnp.where(b_row < b_lane, 1.0, 0.0),
                jnp.ones((16, 128), F32),
            ],
            axis=1,
        )
        counted = jnp.dot(onehot, spread, preferred_element_type=F32)
        o_col = lax.broadcasted_iota(jnp.int32, (8, 128), 0).astype(F32)
        row_id = lax.broadcasted_iota(jnp.int32, (128, 128), 0).astype(F32)
        previous = jnp.zeros((8, 128), F32)
        edge = jnp.full((1, 128), -1.0, F32)
        for c in range(4):
            here = counted[c * 8 : c * 8 + 8, 0:128]
            before = counted[c * 8 : c * 8 + 8, 128:256] + previous
            previous = previous + counted[c * 8 : c * 8 + 8, 256:384]
            solid = jnp.sum(here, axis=0, keepdims=True)
            slot = jnp.sum(here * (2.0 * o_col + before), axis=0, keepdims=True)
            code = jnp.where(solid > 0.5, slot * 8.0 + (lane_row % 8).astype(F32), -1.0)
            mrow[c : c + 1, :] = solid
            picked = jnp.where(row_id == code, 1.0, 0.0).astype(BF16)
            sel[0:128, c * 128 : (c + 1) * 128] = picked
            sel[128:256, c * 128 : (c + 1) * 128] = picked
            edge = jnp.where(lane_row % 8 == 2 * c, jnp.broadcast_to(code[:, 127:128], (1, 128)), edge)
            edge = jnp.where(lane_row % 8 == 2 * c + 1, jnp.broadcast_to(code[:, 0:1], (1, 128)), edge)
        picked = jnp.where(row_id == edge, 1.0, 0.0).astype(BF16)
        ez[0:128, :] = picked
        ez[128:256, :] = picked

    def halo_copies(it):
        f = field.at[it]
        inner = pl.ds(1, 16)
        copies = []
        for n, (axis, idx, size, src, dst) in enumerate(
            (
                ("span", S, n_span, f.at[16, inner], f.at[0, inner]),
                ("span", S, n_span, f.at[1, inner], f.at[17, inner]),
                ("height", H, n_height, f.at[inner, 16], f.at[inner, 0]),
                ("height", H, n_height, f.at[inner, 1], f.at[inner, 17]),
                ("depth", D, n_depth, hz_s.at[it], hz_r.at[it, 0]),
                ("depth", D, n_depth, hz_s.at[it], hz_r.at[it, 1]),
            )
        ):
            copies.append((axis, idx, size, n % 2, src, dst, halo_ss.at[it, n], halo_rs.at[it, n]))
        return copies

    def small_copies(e):
        f = ext.at[e]
        copies = []
        for n, (axis, idx, size, src, dst) in enumerate(
            (
                ("span", S, n_span, f.at[pl.ds(256, 16)], f.at[pl.ds(0, 16)]),
                ("span", S, n_span, f.at[pl.ds(16, 16)], f.at[pl.ds(272, 16)]),
                ("height", H, n_height, sf_s.at[e, 1], sf_r.at[e, 0]),
                ("height", H, n_height, sf_s.at[e, 0], sf_r.at[e, 1]),
                ("depth", D, n_depth, sf_s.at[e, 2, pl.ds(0, 8)], sf_r.at[e, 2, pl.ds(0, 8)]),
                ("depth", D, n_depth, sf_s.at[e, 2, pl.ds(0, 8)], sf_r.at[e, 2, pl.ds(8, 8)]),
            )
        ):
            copies.append((axis, idx, size, n % 2, src, dst, sf_ss.at[e, n], sf_rs.at[e, n]))
        return copies

    def make(copy):
        axis, idx, size, direction, src, dst, ss, rs = copy
        target = idx + 1 if direction == 0 else idx - 1
        return pltpu.make_async_remote_copy(
            src_ref=src, dst_ref=dst, send_sem=ss, recv_sem=rs,
            device_id={axis: lax.rem(target + size, size)}, device_id_type=MESH,
        )

    def sends(copy):
        _, idx, size, direction = copy[:4]
        return idx < size - 1 if direction == 0 else idx > 0

    def receives(copy):
        _, idx, size, direction = copy[:4]
        return idx > 0 if direction == 0 else idx < size - 1

    def start_all(copies):
        for copy in copies:
            if copy[2] > 1:
                pl.when(sends(copy))(lambda copy=copy: make(copy).start())

    def receive_all(copies):
        for copy in copies:
            if copy[2] > 1:
                pl.when(receives(copy))(lambda copy=copy: make(copy).wait_recv())

    def sent_all(copies):
        for copy in copies:
            if copy[2] > 1:
                pl.when(sends(copy))(lambda copy=copy: make(copy).wait_send())

    def span_copy(src, dst, ss, rs, partner):
        return pltpu.make_async_remote_copy(
            src_ref=src, dst_ref=dst, send_sem=ss, recv_sem=rs,
            device_id={"span": partner}, device_id_type=MESH,
        )

    def a2a_out(it, n):
        to = towards(*PARTNERS[n])
        return span_copy(
            send_a[it].at[to], recv_a[it].at[S], a2a_ss.at[it, n], a2a_rs.at[it, n], to
        )

    def a2a_back(it, n):
        to = back(*PARTNERS[n])
        return span_copy(
            send_r.at[it, to], recv_r.at[it, S], ret_ss.at[it, n], ret_rs.at[it, n], to
        )

    plane = [(h, d) for h in range(n_height) for d in range(n_depth) if h or d]

    def ar_copies(k, stage):
        copies = []
        for n, p in enumerate(PARTNERS if stage == 0 else plane):
            at = n + 7 * stage
            if stage == 0:
                target = {"span": towards(*p)}
            else:
                target = {
                    "height": lax.rem(H + p[0], n_height),
                    "depth": lax.rem(D + p[1], n_depth),
                }
            copies.append(
                pltpu.make_async_remote_copy(
                    src_ref=ar_s.at[k, stage], dst_ref=ar_r.at[k, at],
                    send_sem=ar_ss.at[k, at], recv_sem=ar_rs.at[k, at],
                    device_id=target, device_id_type=MESH,
                )
            )
        return copies

    def ar_begin(k, stage, value):
        ar_s[k, stage] = value
        for c in reversed(ar_copies(k, stage)):
            c.start()

    def ar_end(k, stage, combine):
        copies = ar_copies(k, stage)
        for c in copies:
            c.wait_recv()
        total = ar_s[k, stage]
        for n in range(len(copies)):
            total = combine(total, ar_r[k, 7 * stage + n])
        return total

    def pack_pair(it, x, y, row):
        both = jnp.concatenate([row(x, y), row(x, y + 1)], axis=0)
        high = both.astype(BF16)
        at, column = (x % 8) * 64 + (y % 8) * 8, ((x // 8) * 2 + y // 8) * 128
        if not isinstance(x, int):
            at, column = pl.multiple_of(at, 16), pl.multiple_of(column, 128)
        lb[pl.ds(at, 16), pl.ds(column, 128)] = high
        if it == 1:
            low = (both - high.astype(F32)).astype(BF16)
            lb[pl.ds(at, 16), pl.ds(column + 512, 128)] = low

    def gather(it):
        by_slot = (((1,), (1,)), ((), ()))
        for g in range(4):
            rows, lanes = slice(g * 128, g * 128 + 128), slice(g * 128, g * 128 + 128)
            chosen = lax.dot_general(
                lb[rows, 0:512], sel[0:128, :], by_slot, preferred_element_type=F32
            )
            if it == 1:
                chosen = chosen + lax.dot_general(
                    lb[rows, 512:1024], sel[0:128, :], by_slot, preferred_element_type=F32
                )
            slots = block_transpose([chosen[8 * t : 8 * t + 8, :] for t in range(16)])
            for o in range(8):
                both = jnp.concatenate([slots[2 * o], slots[2 * o + 1]], axis=0)
                high = both.astype(BF16)
                send_a[it][o, 0:16, lanes] = high
                if it == 1:
                    low = (both - high.astype(F32)).astype(BF16)
                    send_a[it][o, 16:32, lanes] = low

    def own_product(it, src, lhs, out):
        for rank in range(2):
            result = jnp.dot(lhs[...], pre_v[src * 2 + rank], preferred_element_type=F32)
            part = result[rank * 8 : rank * 8 + 8, :]
            if it == 1:
                part = part + result[16 + rank * 8 : 24 + rank * 8, :]
            out[rank * 8 : rank * 8 + 8, :] = part

    def precondition(it):
        if it == 0:
            pre_in[0].wait()
        own_product(it, S, send_a[it].at[S], recv_r.at[it, S])
        for n in range(7):
            if it == 0:
                pre_in[n + 1].wait()
            src = sources[n + 1]
            a2a_out(it, n).wait_recv()
            own_product(it, src, recv_a[it].at[src], send_r.at[it, src])
            a2a_back(it, n).start()

    def scatter(it):
        for n in range(7):
            a2a_back(it, n).wait_recv()

        for g in range(4):
            slots = [
                recv_r[it, s // 2, (s % 2) * 8 : (s % 2) * 8 + 8, g * 128 : g * 128 + 128]
                for s in range(16)
            ]
            rows = block_transpose(slots)
            for t in range(0, 16, 2):
                both = jnp.concatenate([rows[t], rows[t + 1]], axis=0)
                high = both.astype(BF16)
                at = slice(g * 128 + 8 * t, g * 128 + 8 * t + 16)
                gbuf[at, 0:128] = high
                gbuf[at, 128:256] = (both - high.astype(F32)).astype(BF16)
            chunk = gbuf[g * 128 : g * 128 + 128, :]
            cells = jnp.dot(chunk, sel[...], preferred_element_type=F32)
            faces = jnp.dot(chunk, ez[...], preferred_element_type=F32)
            packed = jnp.zeros((8, 128), F32)
            for t in range(16):
                ii, j = t // 8, t % 8
                for c in range(4):
                    bx, by = c // 2, c % 2
                    field[it, 1 + 8 * bx + 2 * g + ii, 1 + 8 * by + j] = cells[
                        t * 8 : t * 8 + 8, c * 128 : (c + 1) * 128
                    ]
                packed = jnp.where(lane // 8 == t, faces[t * 8 : t * 8 + 8, :], packed)
            hz_s[it, g] = packed

    def merge(right, left):
        return jnp.where(lane % 2 == 0, pltpu.roll(right, 127, 1), pltpu.roll(left, 1, 1))

    def unrolled(count, step, body):
        def several(g, _):
            for k in range(step):
                body(g * step + k, 0)
            return 0

        lax.fori_loop(0, count // step, several, 0)

    def small_faces(e):
        for side, y in ((0, 0), (1, 15)):
            sf_s[e, side] = ext[e, pl.ds(16 + y, 16, stride=16), :]
        parts = [jnp.zeros((8, 128), F32)] * 4
        for n in range(32):
            rows = pltpu.roll(ext[e, 16 + 8 * n : 24 + 8 * n, :], 2 * n + 1, 1)
            parts[n % 4] = jnp.where(lane // 2 == n, rows, parts[n % 4])
        sf_s[e, 2, 0:8, :] = (parts[0] + parts[1]) + (parts[2] + parts[3])

    def small_merge(e):
        sf_m[e] = merge(sf_r[e, 2, 8:16, :], sf_r[e, 2, 0:8, :])

    sub16 = lax.broadcasted_iota(jnp.int32, (16, 128), 0)
    lane16 = lax.broadcasted_iota(jnp.int32, (16, 128), 1)

    def small_block(e, x):
        return ext[e, pl.ds(pl.multiple_of(x * 16 + 16, 16), 16), :]

    def small_neighbours(e, x):
        mid = small_block(e, x)
        xp = ext[e, pl.ds(pl.multiple_of(x * 16 + 32, 16), 16), :]
        xm = ext[e, pl.ds(pl.multiple_of(x * 16, 16), 16), :]
        low = jnp.broadcast_to(sf_r[e, 0, pl.ds(x, 1), :], (16, 128))
        high = jnp.broadcast_to(sf_r[e, 1, pl.ds(x, 1), :], (16, 128))
        yp = jnp.where(sub16 == 15, high, pltpu.roll(mid, 15, 0))
        ym = jnp.where(sub16 == 0, low, pltpu.roll(mid, 1, 0))
        sides = jnp.concatenate(
            [pltpu.roll(sf_m[e], 127 - 2 * (2 * x + h), 1) for h in range(2)], axis=0
        )
        zp = jnp.where(lane16 == 127, sides, pltpu.roll(mid, 127, 1))
        zm = jnp.where(lane16 == 0, sides, pltpu.roll(mid, 1, 1))
        return xp, xm, yp, ym, zp, zm

    def small_sum(e, x):
        xp, xm, yp, ym, zp, zm = small_neighbours(e, x)
        return xp + xm + yp + ym + zp + zm

    def mask_block(x):
        bx = x // 8
        both = mrow[pl.ds(2 * bx, 2), :]
        return jnp.where(
            sub16 < 8,
            jnp.broadcast_to(both[0:1, :], (16, 128)),
            jnp.broadcast_to(both[1:2, :], (16, 128)),
        )

    def rows_of(x):
        return pl.ds(pl.multiple_of(x * 16, 16), 16)

    def clear_halos():
        zero_plane = jnp.zeros((16, 8, 128), F32)
        zero_face = jnp.zeros((16, 128), F32)

        def clear(cond, fn):
            pl.when(cond)(fn)

        def span_low():
            for it in range(2):
                field[it, 0, 1:17] = zero_plane
            for e in range(4):
                ext[e, 0:16, :] = zero_face

        def span_high():
            for it in range(2):
                field[it, 17, 1:17] = zero_plane
            for e in range(4):
                ext[e, 272:288, :] = zero_face

        def height_low():
            for it in range(2):
                field[it, 1:17, 0] = zero_plane
            for e in range(4):
                sf_r[e, 0] = zero_face

        def height_high():
            for it in range(2):
                field[it, 1:17, 17] = zero_plane
            for e in range(4):
                sf_r[e, 1] = zero_face

        def depth_low():
            for it in range(2):
                hz_r[it, 0] = jnp.zeros((4, 8, 128), F32)
            for e in range(4):
                sf_r[e, 2, 0:8, :] = jnp.zeros((8, 128), F32)

        def depth_high():
            for it in range(2):
                hz_r[it, 1] = jnp.zeros((4, 8, 128), F32)
            for e in range(4):
                sf_r[e, 2, 8:16, :] = jnp.zeros((8, 128), F32)

        clear(S == 0, span_low)
        clear(S == n_span - 1, span_high)
        clear(H == 0, height_low)
        clear(H == n_height - 1, height_high)
        clear(D == 0, depth_low)
        clear(D == n_depth - 1, depth_high)

    def setup_masked_stiffness():
        phase_in.wait()

        def body(x, _):
            p = small_block(1, x)
            stiff = void_stiffness + (1.0 - void_stiffness) * (p * p * p)
            m = mask_block(x)
            ext[0, pl.ds(pl.multiple_of(x * 16 + 16, 16), 16), :] = m * stiff
            rate[rows_of(x), :] = (-1.5 * (1.0 - void_stiffness)) * (p * p) * m

        unrolled(16, 4, body)
        for e in range(2):
            small_faces(e)
            start_all(small_copies(e))

    def setup_coefficients():
        for e in range(2):
            receive_all(small_copies(e))
            small_merge(e)

        def body(x, _):
            p = small_block(1, x)
            stiff = void_stiffness + (1.0 - void_stiffness) * (p * p * p)
            m = mask_block(x)
            half = 0.5 * m
            total = m * spring_rate
            w = []
            for near in small_neighbours(0, x):
                one = half * (jnp.where(near > 0.0, stiff, 0.0) + near)
                total = total + one
                w.append(one)
            at = rows_of(x)
            dco[at, :] = total
            wx[pl.ds(pl.multiple_of(x * 16 + 16, 16), 16), :] = w[0]
            wx[at, :] = w[1]
            wyp[at, :] = w[2]
            wym[at, :] = w[3]
            wzl[at, :] = jnp.where(lane16 == 127, 0.0, w[4])
            wze[at, :] = jnp.where(lane16 == 127, w[4], jnp.where(lane16 == 0, w[5], 0.0))
            b = p / time_step - 0.5 * p * (1.0 - p) * (1.0 - 2.0 * p)
            base[at, :] = b
            ext[2, pl.ds(pl.multiple_of(x * 16 + 16, 16), 16), :] = inverse * (
                b + interface_weight * small_sum(1, x)
            )

        unrolled(16, 4, body)
        small_faces(2)
        start_all(small_copies(2))

    def setup_phase_part():
        receive_all(small_copies(2))
        small_merge(2)

        def body(x, _):
            at = rows_of(x)
            hpart[at, :] = inverse * (base[at, :] + interface_weight * small_sum(2, x))

        unrolled(16, 4, body)

    def load_row(x, y):
        return load_v[pl.ds(x * 16 + y, 8, stride=PITCH), :]

    def side_values(source, x, y):
        n = ((x % 2) * 8 + y % 8) * 4 + (x // 8) * 2 + y // 8
        return pltpu.roll(source, 127 - 2 * n, 1)

    def local(it, x, y, low, high):
        r = pl.ds(x * 16 + y, 1)
        v = field[it, x + 1, y + 1]
        wz = wzl[r, :]
        q = dco[r, :] * v
        if low:
            q = q - wx[r, :] * field[it, x, y + 1]
        if high:
            q = q - wx[pl.ds(x * 16 + 16 + y, 1), :] * field[it, x + 2, y + 1]
        if y > 0:
            q = q - wym[r, :] * field[it, x + 1, y]
        if y < 15:
            q = q - wyp[r, :] * field[it, x + 1, y + 2]
        return v, q - wz * pltpu.roll(v, 127, 1) - pltpu.roll(wz * v, 1, 1)

    def over_planes(body, carry):
        carry = body(0, carry, False, True)
        carry = lax.fori_loop(1, 15, lambda x, c: body(x, c, True, True), carry)
        return body(15, carry, True, False)

    lane_row8 = jnp.broadcast_to(lane_row, (8, 128))
    sub8 = lax.broadcasted_iota(jnp.int32, (8, 128), 0)

    def as_row(*accumulated):
        packed = jnp.zeros((8, 128), F32)
        for n, a in enumerate(accumulated):
            packed = jnp.where(lane_row8 == 8 * n + sub8, jnp.sum(a, axis=1, keepdims=True), packed)
        return jnp.sum(packed, axis=0, keepdims=True)

    def from_row(row, n):
        own = jnp.where(lane_row8 == 8 * n + sub8, jnp.broadcast_to(row, (8, 128)), 0.0)
        return jnp.broadcast_to(jnp.sum(own, axis=1, keepdims=True), (8, 128))

    def receive_depth(it):
        receive_all(halo_copies(it)[4:])
        for g in range(4):
            hz_m[it, g] = merge(hz_r[it, 1, g], hz_r[it, 0, g])

    def pack_edge_weights():
        def body(g, _):
            packed = [jnp.zeros((8, 128), F32)] * 4
            for ii in range(2):
                for c in range(4):
                    x = 8 * (c // 2) + 2 * g + ii
                    for j in range(8):
                        n = (ii * 8 + j) * 4 + c
                        row = wze[pl.ds(x * 16 + 8 * (c % 2) + j, 1), :]
                        row = pltpu.roll(jnp.broadcast_to(row, (8, 128)), 2 * n + 1, 1)
                        packed[c] = jnp.where(lane // 2 == n, row, packed[c])
            wzp[g] = (packed[0] + packed[1]) + (packed[2] + packed[3])
            return 0

        lax.fori_loop(0, 4, body, 0)

    def load_sums(rows):
        first = sub8 < 4
        out = []
        for y in range(4):
            a, b = rows[y], rows[y + 4]
            out.append(jnp.where(first, a, b) + pltpu.roll(jnp.where(first, b, a), 4, 0))
        rows = out
        for half in (2, 1):
            first = (sub8 % (2 * half)) < half
            out = []
            for y in range(half):
                a, b = rows[y], rows[y + half]
                other = jnp.where(first, b, a)
                moved = jnp.where(
                    first, pltpu.roll(other, 8 - half, 0), pltpu.roll(other, half, 0)
                )
                out.append(jnp.where(first, a, b) + moved)
            rows = out
        return rows[0]

    zero = jnp.zeros((8, 128), F32)
    add = lambda a, b: a + b

    for c in load_in:
        c.wait()

    def pack_load(x, _):
        for y in range(0, 16, 2):
            pack_pair(0, x, y, load_row)
        return 0

    lax.fori_loop(0, 16, pack_load, 0)
    plan()
    gather(0)
    pl.semaphore_wait(barrier, 7 + (n_height - 1) + (n_depth - 1))
    for n in range(7):
        a2a_out(0, n).start()
    for d in range(1, n_height):
        pl.semaphore_signal(
            far_sem, 1, device_id={"height": lax.rem(H + d, n_height)}, device_id_type=MESH
        )
    clear_halos()
    setup_masked_stiffness()
    precondition(0)
    setup_coefficients()
    scatter(0)
    start_all(halo_copies(0))

    def local_first(x, carry, low, high):
        for y in range(16):
            image[x, y] = local(0, x, y, low, high)[1]
        return carry

    over_planes(local_first, 0)
    receive_depth(0)

    def image_row(x, y):
        r = pl.ds(x * 16 + y, 1)
        q = image[x, y] - wze[r, :] * side_values(hz_m[0, (x % 8) // 2], x, y)
        if isinstance(x, int) and x == 0:
            q = q - wx[r, :] * field[0, 0, y + 1]
        if isinstance(x, int) and x == 15:
            q = q - wx[pl.ds(256 + y, 1), :] * field[0, 17, y + 1]
        if y == 0:
            q = q - wym[r, :] * field[0, x + 1, 0]
        if y == 15:
            q = q - wyp[r, :] * field[0, x + 1, 17]
        image[x, y] = q
        return q

    def pack_inner(x, _):
        for y in range(2, 14, 2):
            pack_pair(1, x, y, image_row)
        return 0

    def pack_rim(x, _):
        for y in (0, 14):
            pack_pair(1, x, y, image_row)
        return 0

    lax.fori_loop(1, 15, pack_inner, 0)
    receive_all(halo_copies(0)[:4])
    unrolled(14, 7, lambda x, _: pack_rim(x + 1, 0))
    for x in (0, 15):
        for y in range(0, 16, 2):
            pack_pair(1, x, y, image_row)
    gather(1)
    for n in range(7):
        a2a_out(1, n).start()

    def first_sums(x, carry):
        rz, zq = carry
        for y in range(16):
            v = field[0, x + 1, y + 1]
            rz = rz + load_row(x, y) * v
            zq = zq + image[x, y] * v
        return rz, zq

    ar_begin(0, 0, as_row(*lax.fori_loop(0, 16, first_sums, (zero, zero))))
    setup_phase_part()
    pack_edge_weights()
    precondition(1)
    if n_height > 1:
        pl.semaphore_wait(far_sem, n_height - 1)
    ar_begin(0, 1, ar_end(0, 0, add))
    scatter(1)
    start_all(halo_copies(1))
    total = ar_end(0, 1, add)
    rz1 = from_row(total, 0)
    zq1 = from_row(total, 1)
    alpha1 = rz1 / zq1

    def local_second(x, carry, low, high):
        rz, zaz, zq = carry
        for y in range(16):
            w, u = local(1, x, y, low, high)
            q1 = image[x, y]
            z2 = field[0, x + 1, y + 1] - alpha1 * w
            rz = rz + (load_row(x, y) - alpha1 * q1) * z2
            zaz = zaz + z2 * (q1 - alpha1 * u)
            zq = zq + z2 * q1
        return rz, zaz, zq

    rz, zaz, zq = over_planes(local_second, (zero, zero, zero))
    receive_depth(1)
    receive_all(halo_copies(1)[:4])

    def second_direction(x, y):
        return field[0, x + 1, y + 1] - alpha1 * field[1, x + 1, y + 1]

    outer = zero
    for y in range(16):
        outer = outer + second_direction(0, y) * (wx[y : y + 1, :] * field[1, 0, y + 1])
        outer = outer + second_direction(15, y) * (wx[256 + y : 257 + y, :] * field[1, 17, y + 1])
        outer = outer + second_direction(y, 0) * (wym[16 * y : 16 * y + 1, :] * field[1, y + 1, 0])
        outer = outer + second_direction(y, 15) * (
            wyp[16 * y + 15 : 16 * y + 16, :] * field[1, y + 1, 17]
        )
    for g in range(4):
        outer = outer + (hz_s[0, g] - alpha1 * hz_s[1, g]) * (wzp[g] * hz_m[1, g])
    ar_begin(1, 0, as_row(rz, zaz + alpha1 * outer, zq))

    def quadratic(x, _):
        hz0 = hz_m[0, (x % 8) // 2]
        hz1 = hz_m[1, (x % 8) // 2]
        for y in range(16):
            r = pl.ds(x * 16 + y, 1)
            z, w = field[0, x + 1, y + 1], field[1, x + 1, y + 1]
            zz = zw = ww = zero
            for weight, near_z, near_w in (
                (wx[r, :], field[0, x, y + 1], field[1, x, y + 1]),
                (wx[pl.ds(x * 16 + 16 + y, 1), :], field[0, x + 2, y + 1], field[1, x + 2, y + 1]),
                (wym[r, :], field[0, x + 1, y], field[1, x + 1, y]),
                (wyp[r, :], field[0, x + 1, y + 2], field[1, x + 1, y + 2]),
                (wze[r, :], side_values(hz0, x, y), side_values(hz1, x, y)),
            ):
                solid = weight > 0.0
                dz = jnp.where(solid, z - near_z, 0.0)
                dw = jnp.where(solid, w - near_w, 0.0)
                zz, zw, ww = zz + dz * dz, zw + dz * dw, ww + dw * dw
            solid = wzl[r, :] > 0.0
            dz = jnp.where(solid, z - pltpu.roll(z, 127, 1), 0.0)
            dw = jnp.where(solid, w - pltpu.roll(w, 127, 1), 0.0)
            uz, uw = pltpu.roll(dz, 1, 1), pltpu.roll(dw, 1, 1)
            quads[0, x, y] = zz + dz * dz + uz * uz
            quads[1, x, y] = zw + dz * dw + uz * uw
            quads[2, x, y] = ww + dw * dw + uw * uw
        return 0

    lax.fori_loop(0, 8, quadratic, 0)
    ar_begin(1, 1, ar_end(1, 0, add))
    lax.fori_loop(8, 16, quadratic, 0)
    total = ar_end(1, 1, add)
    rz2 = from_row(total, 0)
    zaz = from_row(total, 1)
    zq2 = from_row(total, 2)
    beta = rz2 / rz1
    alpha2 = rz2 / (zaz + beta * (2.0 * zq2 + beta * zq1))
    on_z = alpha1 + alpha2 * (1.0 + beta)
    on_w = -alpha2 * alpha1
    on_zz, on_zw, on_ww = on_z * on_z, 2.0 * on_z * on_w, on_w * on_w

    def sensitivities(x, peak):
        for h in range(2):
            energy = load_sums(
                [
                    on_zz * quads[0, x, 8 * h + y]
                    + on_zw * quads[1, x, 8 * h + y]
                    + on_ww * quads[2, x, 8 * h + y]
                    for y in range(8)
                ]
            )
            at = pl.multiple_of(x * 16, 16) + 8 * h
            s = rate[pl.ds(at, 8), :] * energy
            sens[pl.ds(at, 8), :] = s
            ext[3, pl.ds(at + 16, 8), :] = inverse * s
            peak = jnp.maximum(peak, -s)
        return peak

    peak = lax.fori_loop(0, 16, sensitivities, zero)
    ar_begin(2, 0, jnp.max(peak, axis=0, keepdims=True))
    small_faces(3)
    start_all(small_copies(3))

    def form(x, _):
        for y in range(16):
            dx[pl.ds(x * 16 + y, 8, stride=PITCH), :] = (
                on_z * field[0, x + 1, y + 1] + on_w * field[1, x + 1, y + 1]
            )
        return 0

    lax.fori_loop(0, 16, form, 0)
    ar_begin(2, 1, ar_end(2, 0, jnp.maximum))
    receive_all(small_copies(3))
    small_merge(3)

    def slopes(x, _):
        slope[rows_of(x), :] = small_block(3, x) + (interface_weight * inverse) * small_sum(3, x)

    unrolled(16, 4, slopes)
    peak = jnp.max(ar_end(2, 1, jnp.maximum), axis=1, keepdims=True)
    scale = jnp.broadcast_to(1.0 / (peak + epsilon_peak), (8, 128))
    for n in range(32):
        at = slice(8 * n, 8 * n + 8)
        nxt[at, :] = hpart[at, :] - slope[at, :] * scale

    for it in range(2):
        for n in range(7):
            a2a_out(it, n).wait_send()
            a2a_back(it, n).wait_send()
        sent_all(halo_copies(it))
    for e in range(4):
        sent_all(small_copies(e))
    for k in range(3):
        for stage in range(2):
            for c in ar_copies(k, stage):
                c.wait_send()


def deliver(dx, sens, nxt, disp_hbm, sens_hbm, next_hbm, sem):
    copies = [
        pltpu.make_async_copy(
            dx.at[pl.ds(l * PITCH, 256)], disp_hbm.at[pl.ds(l * 256, 256)], sem.at[l]
        )
        for l in range(8)
    ]
    copies.append(pltpu.make_async_copy(sens, sens_hbm, sem.at[8]))
    copies.append(pltpu.make_async_copy(nxt, next_hbm, sem.at[9]))
    for c in copies:
        c.start()
    for c in copies:
        c.wait()


def solution(mesh):
    sizes = tuple(mesh.shape[a] for a in AXES)
    dma = pltpu.SemaphoreType.DMA
    vmem = pltpu.VMEM

    def local(load, phase, void, owner, precond):
        vmem_space = pl.BlockSpec(memory_space=pltpu.VMEM)
        hbm_space = pl.BlockSpec(memory_space=pltpu.HBM)
        results = pl.pallas_call(
            functools.partial(kernel, sizes),
            name="design_step",
            out_shape=(
                jax.ShapeDtypeStruct((8 * PITCH, 128), F32),
                jax.ShapeDtypeStruct((256, 128), F32),
                jax.ShapeDtypeStruct((256, 128), F32),
            ),
            in_specs=[hbm_space] * 5,
            out_specs=(vmem_space,) * 3,
            scratch_shapes=[
                vmem((8 * PITCH, 128), F32),
                vmem((2, 2, 16), jnp.int32),
                vmem((2, 2, 16), jnp.int32),
                vmem((16, 512, 512), BF16),
                vmem((256, 512), BF16),
                vmem((256, 128), BF16),
                vmem((8, 128), F32),
                vmem((512, 1024), BF16),
                vmem((512, 256), BF16),
                vmem((8, 16, 512), BF16),
                vmem((8, 32, 512), BF16),
                vmem((8, 16, 512), BF16),
                vmem((8, 32, 512), BF16),
                vmem((2, 8, 16, 512), F32),
                vmem((2, 8, 16, 512), F32),
                vmem((2, 18, 18, 8, 128), F32),
                vmem((16, 16, 8, 128), F32),
                vmem((3, 16, 16, 8, 128), F32),
                vmem((2, 4, 8, 128), F32),
                vmem((2, 2, 4, 8, 128), F32),
                vmem((2, 4, 8, 128), F32),
                vmem((4, 8, 128), F32),
                vmem((4, 288, 128), F32),
                vmem((4, 3, 16, 128), F32),
                vmem((4, 3, 16, 128), F32),
                vmem((4, 8, 128), F32),
                vmem((256, 128), F32),
                vmem((272, 128), F32),
                vmem((256, 128), F32),
                vmem((256, 128), F32),
                vmem((256, 128), F32),
                vmem((256, 128), F32),
                vmem((256, 128), F32),
                vmem((256, 128), F32),
                vmem((256, 128), F32),
                vmem((256, 128), F32),
                vmem((3, 2, 1, 128), F32),
                vmem((3, 22, 1, 128), F32),
                dma((11,)),
                dma((8,)),
                dma((2, 7)),
                dma((2, 7)),
                dma((2, 7)),
                dma((2, 7)),
                dma((2, 6)),
                dma((2, 6)),
                dma((4, 6)),
                dma((4, 6)),
                dma((3, 22)),
                dma((3, 22)),
                pltpu.SemaphoreType.REGULAR,
            ],
            compiler_params=pltpu.CompilerParams(
                collective_id=0, has_side_effects=True, vmem_limit_bytes=48 * 2**20
            ),
        )(*(
            pltpu.with_memory_space_constraint(a, pltpu.HBM)
            for a in (load.reshape(2048, 128), phase.reshape(256, 128), void, owner, precond)
        ))
        disp, sens, nxt = pl.pallas_call(
            deliver,
            name="deliver",
            out_shape=(
                jax.ShapeDtypeStruct((2048, 128), F32),
                jax.ShapeDtypeStruct((256, 128), F32),
                jax.ShapeDtypeStruct((256, 128), F32),
            ),
            in_specs=[pl.BlockSpec(memory_space=pl.ANY)] * 3,
            out_specs=(hbm_space,) * 3,
            scratch_shapes=[dma((10,))],
            compiler_params=pltpu.CompilerParams(vmem_limit_bytes=2**20),
        )(*results)
        return (
            disp.reshape(8, 16, 16, 128),
            sens.reshape(16, 16, 128),
            nxt.reshape(16, 16, 128),
        )

    return jax.shard_map(
        local,
        mesh=mesh,
        in_specs=(P(None, *AXES), P(*AXES), P(*AXES), P(*AXES), P(AXES, None, None)),
        out_specs=(P(None, *AXES), P(*AXES), P(*AXES)),
        check_vma=False,
    )
```

```python
import functools

import jax
import jax.numpy as jnp
from jax import lax
from jax.experimental import pallas as pl
from jax.experimental.pallas import tpu as pltpu
from jax.sharding import PartitionSpec as P

AXES = ("span", "height", "depth")
MESH = pl.DeviceIdType.MESH
F32 = jnp.float32
BF16 = jnp.bfloat16

void_stiffness = 0.001
spring_rate = 0.05
time_step = 0.5
interface_weight = 0.5
epsilon_peak = 1e-06
inverse = 1.0 / (1.0 / time_step + 6.0 * interface_weight)

PITCH = 264

PARTNERS = ((0, 1), (1, 0), (3, 0), (1, 1), (3, 1), (2, 0), (2, 1))


def block_transpose(rows):
    lane_block = lax.broadcasted_iota(jnp.int32, (8, 128), 1) // 8
    rows = [pltpu.roll(r, 8 * t, 1) if t else r for t, r in enumerate(rows)]
    for bit in (1, 2, 4, 8):
        taken = (lane_block % (2 * bit)) >= bit
        rows = [jnp.where(taken, rows[(t + bit) % 16], rows[t]) for t in range(16)]
    out = []
    for s in range(16):
        r = rows[(16 - s) % 16]
        out.append(pltpu.roll(r, 128 - 8 * s, 1) if s else r)
    return out


def kernel(
    sizes,
    load_hbm, phase_hbm, void_hbm, owner_hbm, precond_hbm,
    dx, sens, nxt,
    load_v, void_v, owner_v, pre_v, sel, ez, mrow, lb, gbuf,
    send_a0, send_a1, recv_a0, recv_a1, send_r, recv_r, field, image, quads, hz_s, hz_r, hz_m, wzp,
    ext, sf_s, sf_r, sf_m, dco, wx, wyp, wym, wzl, wze, base, hpart, slope, rate, ar_s, ar_r,
    in_sem, pre_sem, a2a_ss, a2a_rs, ret_ss, ret_rs, halo_ss, halo_rs,
    sf_ss, sf_rs, ar_ss, ar_rs, far_sem,
):
    n_span, n_height, n_depth = sizes
    send_a, recv_a = (send_a0, send_a1), (recv_a0, recv_a1)
    S, H, D = (lax.axis_index(a) for a in AXES)
    yy, core = S // 2, S % 2
    lane = lax.broadcasted_iota(jnp.int32, (8, 128), 1)

    def towards(dy, dc):
        return lax.rem(yy + dy, 4) * 2 + (1 - core if dc else core)

    def back(dy, dc):
        return lax.rem(yy + 4 - dy, 4) * 2 + (1 - core if dc else core)

    load_in = [
        pltpu.make_async_copy(
            load_hbm.at[pl.ds(l * 256, 256)], load_v.at[pl.ds(l * PITCH, 256)], in_sem.at[l]
        )
        for l in range(8)
    ]
    void_in = pltpu.make_async_copy(void_hbm, void_v, in_sem.at[8])
    owner_in = pltpu.make_async_copy(owner_hbm, owner_v, in_sem.at[9])
    phase_in = pltpu.make_async_copy(phase_hbm, ext.at[1, pl.ds(16, 256)], in_sem.at[10])
    void_in.start()
    owner_in.start()
    for c in load_in:
        c.start()
    phase_in.start()

    barrier = pltpu.get_barrier_semaphore()
    for dy, dc in PARTNERS:
        pl.semaphore_signal(barrier, 1, device_id={"span": towards(dy, dc)}, device_id_type=MESH)
    for d in range(1, n_height):
        pl.semaphore_signal(
            barrier, 1, device_id={"height": lax.rem(H + d, n_height)}, device_id_type=MESH
        )
    for d in range(1, n_depth):
        pl.semaphore_signal(
            barrier, 1, device_id={"depth": lax.rem(D + d, n_depth)}, device_id_type=MESH
        )

    sources = [S] + [back(dy, dc) for dy, dc in PARTNERS]
    pre_in = [
        pltpu.make_async_copy(
            precond_hbm.at[pl.ds(src * 2, 2)], pre_v.at[pl.ds(src * 2, 2)], pre_sem.at[n]
        )
        for n, src in enumerate(sources)
    ]
    lane_row = lax.broadcasted_iota(jnp.int32, (1, 128), 1)

    def plan():
        void_in.wait()
        owner_in.wait()
        o_row = lax.broadcasted_iota(jnp.int32, (8, 16), 0)
        onehots = []
        for bx in range(2):
            own2, solid2 = owner_v[bx], 1 - void_v[bx]
            for by in range(2):
                own_row = jnp.broadcast_to(own2[by : by + 1, :], (8, 16))
                sol_row = jnp.broadcast_to(solid2[by : by + 1, :], (8, 16))
                onehots.append(jnp.where((own_row == o_row) & (sol_row == 1), 1.0, 0.0))
        onehot = jnp.concatenate(onehots, axis=0)
        b_row = lax.broadcasted_iota(jnp.int32, (16, 128), 0)
        b_lane = lax.broadcasted_iota(jnp.int32, (16, 128), 1) // 8
        spread = jnp.concatenate(
            [
                jnp.where(b_row == b_lane, 1.0, 0.0),
                jnp.where(b_row < b_lane, 1.0, 0.0),
                jnp.ones((16, 128), F32),
            ],
            axis=1,
        )
        counted = jnp.dot(onehot, spread, preferred_element_type=F32)
        o_col = lax.broadcasted_iota(jnp.int32, (8, 128), 0).astype(F32)
        row_id = lax.broadcasted_iota(jnp.int32, (128, 128), 0).astype(F32)
        previous = jnp.zeros((8, 128), F32)
        edge = jnp.full((1, 128), -1.0, F32)
        for c in range(4):
            here = counted[c * 8 : c * 8 + 8, 0:128]
            before = counted[c * 8 : c * 8 + 8, 128:256] + previous
            previous = previous + counted[c * 8 : c * 8 + 8, 256:384]
            solid = jnp.sum(here, axis=0, keepdims=True)
            slot = jnp.sum(here * (2.0 * o_col + before), axis=0, keepdims=True)
            code = jnp.where(solid > 0.5, slot * 8.0 + (lane_row % 8).astype(F32), -1.0)
            mrow[c : c + 1, :] = solid
            picked = jnp.where(row_id == code, 1.0, 0.0).astype(BF16)
            sel[0:128, c * 128 : (c + 1) * 128] = picked
            sel[128:256, c * 128 : (c + 1) * 128] = picked
            edge = jnp.where(lane_row % 8 == 2 * c, jnp.broadcast_to(code[:, 127:128], (1, 128)), edge)
            edge = jnp.where(lane_row % 8 == 2 * c + 1, jnp.broadcast_to(code[:, 0:1], (1, 128)), edge)
        picked = jnp.where(row_id == edge, 1.0, 0.0).astype(BF16)
        ez[0:128, :] = picked
        ez[128:256, :] = picked

    def halo_copies(it):
        f = field.at[it]
        inner = pl.ds(1, 16)
        copies = []
        for n, (axis, idx, size, src, dst) in enumerate(
            (
                ("span", S, n_span, f.at[16, inner], f.at[0, inner]),
                ("span", S, n_span, f.at[1, inner], f.at[17, inner]),
                ("height", H, n_height, f.at[inner, 16], f.at[inner, 0]),
                ("height", H, n_height, f.at[inner, 1], f.at[inner, 17]),
                ("depth", D, n_depth, hz_s.at[it], hz_r.at[it, 0]),
                ("depth", D, n_depth, hz_s.at[it], hz_r.at[it, 1]),
            )
        ):
            copies.append((axis, idx, size, n % 2, src, dst, halo_ss.at[it, n], halo_rs.at[it, n]))
        return copies

    def small_copies(e):
        f = ext.at[e]
        copies = []
        for n, (axis, idx, size, src, dst) in enumerate(
            (
                ("span", S, n_span, f.at[pl.ds(256, 16)], f.at[pl.ds(0, 16)]),
                ("span", S, n_span, f.at[pl.ds(16, 16)], f.at[pl.ds(272, 16)]),
                ("height", H, n_height, sf_s.at[e, 1], sf_r.at[e, 0]),
                ("height", H, n_height, sf_s.at[e, 0], sf_r.at[e, 1]),
                ("depth", D, n_depth, sf_s.at[e, 2, pl.ds(0, 8)], sf_r.at[e, 2, pl.ds(0, 8)]),
                ("depth", D, n_depth, sf_s.at[e, 2, pl.ds(0, 8)], sf_r.at[e, 2, pl.ds(8, 8)]),
            )
        ):
            copies.append((axis, idx, size, n % 2, src, dst, sf_ss.at[e, n], sf_rs.at[e, n]))
        return copies

    def make(copy):
        axis, idx, size, direction, src, dst, ss, rs = copy
        target = idx + 1 if direction == 0 else idx - 1
        return pltpu.make_async_remote_copy(
            src_ref=src, dst_ref=dst, send_sem=ss, recv_sem=rs,
            device_id={axis: lax.rem(target + size, size)}, device_id_type=MESH,
        )

    def sends(copy):
        _, idx, size, direction = copy[:4]
        return idx < size - 1 if direction == 0 else idx > 0

    def receives(copy):
        _, idx, size, direction = copy[:4]
        return idx > 0 if direction == 0 else idx < size - 1

    def start_all(copies):
        for copy in copies:
            if copy[2] > 1:
                pl.when(sends(copy))(lambda copy=copy: make(copy).start())

    def receive_all(copies):
        for copy in copies:
            if copy[2] > 1:
                pl.when(receives(copy))(lambda copy=copy: make(copy).wait_recv())

    def sent_all(copies):
        for copy in copies:
            if copy[2] > 1:
                pl.when(sends(copy))(lambda copy=copy: make(copy).wait_send())

    def span_copy(src, dst, ss, rs, partner):
        return pltpu.make_async_remote_copy(
            src_ref=src, dst_ref=dst, send_sem=ss, recv_sem=rs,
            device_id={"span": partner}, device_id_type=MESH,
        )

    def a2a_out(it, n):
        to = towards(*PARTNERS[n])
        return span_copy(
            send_a[it].at[to], recv_a[it].at[S], a2a_ss.at[it, n], a2a_rs.at[it, n], to
        )

    def a2a_back(it, n):
        to = back(*PARTNERS[n])
        return span_copy(
            send_r.at[it, to], recv_r.at[it, S], ret_ss.at[it, n], ret_rs.at[it, n], to
        )

    plane = [(h, d) for h in range(n_height) for d in range(n_depth) if h or d]

    def ar_copies(k, stage):
        copies = []
        for n, p in enumerate(PARTNERS if stage == 0 else plane):
            at = n + 7 * stage
            if stage == 0:
                target = {"span": towards(*p)}
            else:
                target = {
                    "height": lax.rem(H + p[0], n_height),
                    "depth": lax.rem(D + p[1], n_depth),
                }
            copies.append(
                pltpu.make_async_remote_copy(
                    src_ref=ar_s.at[k, stage], dst_ref=ar_r.at[k, at],
                    send_sem=ar_ss.at[k, at], recv_sem=ar_rs.at[k, at],
                    device_id=target, device_id_type=MESH,
                )
            )
        return copies

    def ar_begin(k, stage, value):
        ar_s[k, stage] = value
        for c in reversed(ar_copies(k, stage)):
            c.start()

    def ar_end(k, stage, combine):
        copies = ar_copies(k, stage)
        for c in copies:
            c.wait_recv()
        total = ar_s[k, stage]
        for n in range(len(copies)):
            total = combine(total, ar_r[k, 7 * stage + n])
        return total

    def pack_pair(it, x, y, upper, lower):
        both = jnp.concatenate([upper, lower], axis=0)
        high = both.astype(BF16)
        if isinstance(x, tuple):
            bx, pair, side = x
            at = pl.multiple_of(pair * 128, 128) + side * 64 + (y % 8) * 8
            column = (bx * 2 + y // 8) * 128
        else:
            at, column = (x % 8) * 64 + (y % 8) * 8, ((x // 8) * 2 + y // 8) * 128
            if not isinstance(x, int):
                at, column = pl.multiple_of(at, 16), pl.multiple_of(column, 128)
        lb[pl.ds(at, 16), pl.ds(column, 128)] = high
        if it == 1:
            low = (both - high.astype(F32)).astype(BF16)
            lb[pl.ds(at, 16), pl.ds(column + 512, 128)] = low

    def gather(it):
        by_slot = (((1,), (1,)), ((), ()))
        for g in range(4):
            rows, lanes = slice(g * 128, g * 128 + 128), slice(g * 128, g * 128 + 128)
            chosen = lax.dot_general(
                lb[rows, 0:512], sel[0:128, :], by_slot, preferred_element_type=F32
            )
            if it == 1:
                chosen = chosen + lax.dot_general(
                    lb[rows, 512:1024], sel[0:128, :], by_slot, preferred_element_type=F32
                )
            slots = block_transpose([chosen[8 * t : 8 * t + 8, :] for t in range(16)])
            for o in range(8):
                pair = slots[2 * o : 2 * o + 2]
                if it == 0:
                    send_a[it][o, :, lanes] = jnp.concatenate(pair, axis=0).astype(BF16)
                    continue
                for rank in range(2):
                    high = pair[rank].astype(BF16).astype(F32)
                    send_a[it][o, rank * 16 : rank * 16 + 16, lanes] = jnp.concatenate(
                        [high, pair[rank] - high], axis=0
                    ).astype(BF16)

    def own_product(it, src, lhs, out):
        for rank in range(2):
            rows = lhs[...] if it == 0 else lhs[rank * 16 : rank * 16 + 16, :]
            result = jnp.dot(rows, pre_v[src * 2 + rank], preferred_element_type=F32)
            if it == 0:
                part = result[rank * 8 : rank * 8 + 8, :]
            else:
                part = result[0:8, :] + result[8:16, :]
            out[rank * 8 : rank * 8 + 8, :] = part

    def precondition(it):
        if it == 0:
            pre_in[0].wait()
        own_product(it, S, send_a[it].at[S], recv_r.at[it, S])
        for n in range(7):
            if it == 0:
                pre_in[n + 1].wait()
            src = sources[n + 1]
            a2a_out(it, n).wait_recv()
            own_product(it, src, recv_a[it].at[src], send_r.at[it, src])
            a2a_back(it, n).start()

    def scatter(it):
        for n in range(7):
            a2a_back(it, n).wait_recv()

        for g in range(4):
            slots = [
                recv_r[it, s // 2, (s % 2) * 8 : (s % 2) * 8 + 8, g * 128 : g * 128 + 128]
                for s in range(16)
            ]
            rows = block_transpose(slots)
            for t in range(0, 16, 2):
                both = jnp.concatenate([rows[t], rows[t + 1]], axis=0)
                high = both.astype(BF16)
                at = slice(g * 128 + 8 * t, g * 128 + 8 * t + 16)
                gbuf[at, 0:128] = high
                gbuf[at, 128:256] = (both - high.astype(F32)).astype(BF16)
            chunk = gbuf[g * 128 : g * 128 + 128, :]
            cells = jnp.dot(chunk, sel[...], preferred_element_type=F32)
            faces = jnp.dot(chunk, ez[...], preferred_element_type=F32)
            packed = jnp.zeros((8, 128), F32)
            for t in range(16):
                ii, j = t // 8, t % 8
                for c in range(4):
                    bx, by = c // 2, c % 2
                    field[it, 1 + 8 * bx + 2 * g + ii, 1 + 8 * by + j] = cells[
                        t * 8 : t * 8 + 8, c * 128 : (c + 1) * 128
                    ]
                packed = jnp.where(lane // 8 == t, faces[t * 8 : t * 8 + 8, :], packed)
            hz_s[it, g] = packed

    def merge(right, left):
        return jnp.where(lane % 2 == 0, pltpu.roll(right, 127, 1), pltpu.roll(left, 1, 1))

    def unrolled(count, step, body):
        def several(g, _):
            for k in range(step):
                body(g * step + k, 0)
            return 0

        lax.fori_loop(0, count // step, several, 0)

    def small_faces(e):
        for side, y in ((0, 0), (1, 15)):
            sf_s[e, side] = ext[e, pl.ds(16 + y, 16, stride=16), :]
        parts = [jnp.zeros((8, 128), F32)] * 4
        for n in range(32):
            rows = pltpu.roll(ext[e, 16 + 8 * n : 24 + 8 * n, :], 2 * n + 1, 1)
            parts[n % 4] = jnp.where(lane // 2 == n, rows, parts[n % 4])
        sf_s[e, 2, 0:8, :] = (parts[0] + parts[1]) + (parts[2] + parts[3])

    def small_merge(e):
        sf_m[e] = merge(sf_r[e, 2, 8:16, :], sf_r[e, 2, 0:8, :])

    sub16 = lax.broadcasted_iota(jnp.int32, (16, 128), 0)
    lane16 = lax.broadcasted_iota(jnp.int32, (16, 128), 1)

    def small_block(e, x):
        return ext[e, pl.ds(pl.multiple_of(x * 16 + 16, 16), 16), :]

    def small_neighbours(e, x):
        mid = small_block(e, x)
        xp = ext[e, pl.ds(pl.multiple_of(x * 16 + 32, 16), 16), :]
        xm = ext[e, pl.ds(pl.multiple_of(x * 16, 16), 16), :]
        low = jnp.broadcast_to(sf_r[e, 0, pl.ds(x, 1), :], (16, 128))
        high = jnp.broadcast_to(sf_r[e, 1, pl.ds(x, 1), :], (16, 128))
        yp = jnp.where(sub16 == 15, high, pltpu.roll(mid, 15, 0))
        ym = jnp.where(sub16 == 0, low, pltpu.roll(mid, 1, 0))
        sides = jnp.concatenate(
            [pltpu.roll(sf_m[e], 127 - 2 * (2 * x + h), 1) for h in range(2)], axis=0
        )
        zp = jnp.where(lane16 == 127, sides, pltpu.roll(mid, 127, 1))
        zm = jnp.where(lane16 == 0, sides, pltpu.roll(mid, 1, 1))
        return xp, xm, yp, ym, zp, zm

    def small_sum(e, x):
        xp, xm, yp, ym, zp, zm = small_neighbours(e, x)
        return xp + xm + yp + ym + zp + zm

    def mask_block(x):
        bx = x // 8
        both = mrow[pl.ds(2 * bx, 2), :]
        return jnp.where(
            sub16 < 8,
            jnp.broadcast_to(both[0:1, :], (16, 128)),
            jnp.broadcast_to(both[1:2, :], (16, 128)),
        )

    def rows_of(x):
        return pl.ds(pl.multiple_of(x * 16, 16), 16)

    def clear_halos():
        zero_plane = jnp.zeros((16, 8, 128), F32)
        zero_face = jnp.zeros((16, 128), F32)

        def clear(cond, fn):
            pl.when(cond)(fn)

        def span_low():
            for it in range(2):
                field[it, 0, 1:17] = zero_plane
            for e in range(4):
                ext[e, 0:16, :] = zero_face

        def span_high():
            for it in range(2):
                field[it, 17, 1:17] = zero_plane
            for e in range(4):
                ext[e, 272:288, :] = zero_face

        def height_low():
            for it in range(2):
                field[it, 1:17, 0] = zero_plane
            for e in range(4):
                sf_r[e, 0] = zero_face

        def height_high():
            for it in range(2):
                field[it, 1:17, 17] = zero_plane
            for e in range(4):
                sf_r[e, 1] = zero_face

        def depth_low():
            for it in range(2):
                hz_r[it, 0] = jnp.zeros((4, 8, 128), F32)
            for e in range(4):
                sf_r[e, 2, 0:8, :] = jnp.zeros((8, 128), F32)

        def depth_high():
            for it in range(2):
                hz_r[it, 1] = jnp.zeros((4, 8, 128), F32)
            for e in range(4):
                sf_r[e, 2, 8:16, :] = jnp.zeros((8, 128), F32)

        clear(S == 0, span_low)
        clear(S == n_span - 1, span_high)
        clear(H == 0, height_low)
        clear(H == n_height - 1, height_high)
        clear(D == 0, depth_low)
        clear(D == n_depth - 1, depth_high)

    def setup_masked_stiffness():
        phase_in.wait()

        def body(x, _):
            p = small_block(1, x)
            stiff = void_stiffness + (1.0 - void_stiffness) * (p * p * p)
            m = mask_block(x)
            ext[0, pl.ds(pl.multiple_of(x * 16 + 16, 16), 16), :] = m * stiff
            rate[rows_of(x), :] = (-1.5 * (1.0 - void_stiffness)) * (p * p) * m

        unrolled(16, 4, body)
        for e in range(2):
            small_faces(e)
            start_all(small_copies(e))

    def setup_coefficients():
        for e in range(2):
            receive_all(small_copies(e))
            small_merge(e)

        def body(x, _):
            p = small_block(1, x)
            stiff = void_stiffness + (1.0 - void_stiffness) * (p * p * p)
            m = mask_block(x)
            half = 0.5 * m
            total = m * spring_rate
            w = []
            for near in small_neighbours(0, x):
                one = half * (jnp.where(near > 0.0, stiff, 0.0) + near)
                total = total + one
                w.append(one)
            at = rows_of(x)
            dco[at, :] = total
            wx[pl.ds(pl.multiple_of(x * 16 + 16, 16), 16), :] = w[0]
            wx[at, :] = w[1]
            wyp[at, :] = w[2]
            wym[at, :] = w[3]
            wzl[at, :] = jnp.where(lane16 == 127, 0.0, w[4])
            wze[at, :] = jnp.where(lane16 == 127, w[4], jnp.where(lane16 == 0, w[5], 0.0))
            b = p / time_step - 0.5 * p * (1.0 - p) * (1.0 - 2.0 * p)
            base[at, :] = b
            ext[2, pl.ds(pl.multiple_of(x * 16 + 16, 16), 16), :] = inverse * (
                b + interface_weight * small_sum(1, x)
            )

        unrolled(16, 4, body)
        small_faces(2)
        start_all(small_copies(2))

    def setup_phase_part():
        receive_all(small_copies(2))
        small_merge(2)

        def body(x, _):
            at = rows_of(x)
            hpart[at, :] = inverse * (base[at, :] + interface_weight * small_sum(2, x))

        unrolled(16, 4, body)

    def load_row(x, y):
        return load_v[pl.ds(x * 16 + y, 8, stride=PITCH), :]

    def side_values(source, x, y):
        n = ((x % 2) * 8 + y % 8) * 4 + (x // 8) * 2 + y // 8
        return pltpu.roll(source, 127 - 2 * n, 1)

    def local(it, x, y, low, high):
        r = pl.ds(x * 16 + y, 1)
        v = field[it, x + 1, y + 1]
        wz = wzl[r, :]
        q = dco[r, :] * v
        if low:
            q = q - wx[r, :] * field[it, x, y + 1]
        if high:
            q = q - wx[pl.ds(x * 16 + 16 + y, 1), :] * field[it, x + 2, y + 1]
        if y > 0:
            q = q - wym[r, :] * field[it, x + 1, y]
        if y < 15:
            q = q - wyp[r, :] * field[it, x + 1, y + 2]
        return v, q - wz * pltpu.roll(v, 127, 1) - pltpu.roll(wz * v, 1, 1)

    def over_planes(body, carry):
        carry = body(0, carry, False, True)
        carry = lax.fori_loop(1, 15, lambda x, c: body(x, c, True, True), carry)
        return body(15, carry, True, False)

    lane_row8 = jnp.broadcast_to(lane_row, (8, 128))
    sub8 = lax.broadcasted_iota(jnp.int32, (8, 128), 0)

    def as_row(*accumulated):
        packed = jnp.zeros((8, 128), F32)
        for n, a in enumerate(accumulated):
            packed = jnp.where(lane_row8 == 8 * n + sub8, jnp.sum(a, axis=1, keepdims=True), packed)
        return jnp.sum(packed, axis=0, keepdims=True)

    def from_row(row, n):
        own = jnp.where(lane_row8 == 8 * n + sub8, jnp.broadcast_to(row, (8, 128)), 0.0)
        return jnp.broadcast_to(jnp.sum(own, axis=1, keepdims=True), (8, 128))

    def receive_depth(it):
        receive_all(halo_copies(it)[4:])
        for g in range(4):
            hz_m[it, g] = merge(hz_r[it, 1, g], hz_r[it, 0, g])

    def pack_edge_weights():
        def body(g, _):
            packed = [jnp.zeros((8, 128), F32)] * 4
            for ii in range(2):
                for c in range(4):
                    x = 8 * (c // 2) + 2 * g + ii
                    for j in range(8):
                        n = (ii * 8 + j) * 4 + c
                        row = wze[pl.ds(x * 16 + 8 * (c % 2) + j, 1), :]
                        row = pltpu.roll(jnp.broadcast_to(row, (8, 128)), 2 * n + 1, 1)
                        packed[c] = jnp.where(lane // 2 == n, row, packed[c])
            wzp[g] = (packed[0] + packed[1]) + (packed[2] + packed[3])
            return 0

        lax.fori_loop(0, 4, body, 0)

    def load_sums(rows):
        first = sub8 < 4
        out = []
        for y in range(4):
            a, b = rows[y], rows[y + 4]
            out.append(jnp.where(first, a, b) + pltpu.roll(jnp.where(first, b, a), 4, 0))
        rows = out
        for half in (2, 1):
            first = (sub8 % (2 * half)) < half
            out = []
            for y in range(half):
                a, b = rows[y], rows[y + half]
                other = jnp.where(first, b, a)
                moved = jnp.where(
                    first, pltpu.roll(other, 8 - half, 0), pltpu.roll(other, half, 0)
                )
                out.append(jnp.where(first, a, b) + moved)
            rows = out
        return rows[0]

    zero = jnp.zeros((8, 128), F32)
    add = lambda a, b: a + b

    for c in load_in:
        c.wait()
    for c in pre_in:
        c.start()

    def pack_load(x, _):
        for y in range(0, 16, 2):
            pack_pair(0, x, y, load_row(x, y), load_row(x, y + 1))
        return 0

    lax.fori_loop(0, 16, pack_load, 0)
    plan()
    gather(0)
    pl.semaphore_wait(barrier, 7 + (n_height - 1) + (n_depth - 1))
    for n in range(7):
        a2a_out(0, n).start()
    for d in range(1, n_height):
        pl.semaphore_signal(
            far_sem, 1, device_id={"height": lax.rem(H + d, n_height)}, device_id_type=MESH
        )
    clear_halos()
    setup_masked_stiffness()
    precondition(0)
    setup_coefficients()
    scatter(0)
    start_all(halo_copies(0))

    def local_first(x, carry, low, high):
        for y in range(16):
            image[x, y] = local(0, x, y, low, high)[1]
        return carry

    over_planes(local_first, 0)
    receive_depth(0)

    def pack_inner(pair, _):
        sides = hz_m[0, pair]
        for bx in range(2):
            for side in range(2):
                x = 8 * bx + 2 * pair + side
                for y in range(0, 16, 2):
                    q = []
                    for k in range(2):
                        n = (side * 8 + (y + k) % 8) * 4 + bx * 2 + y // 8
                        edge = wze[pl.ds(pair * 32 + (8 * bx + side) * 16 + y + k, 1), :]
                        q.append(image[x, y + k] - edge * pltpu.roll(sides, 127 - 2 * n, 1))
                        image[x, y + k] = q[k]
                    pack_pair(1, (bx, pair, side), y, *q)
        return 0

    lax.fori_loop(0, 4, pack_inner, 0)
    receive_all(halo_copies(0)[:4])

    def rim_row(x, y):
        r = slice(16 * x + y, 16 * x + y + 1)
        q = image[x, y]
        if x == 0:
            q = q - wx[r, :] * field[0, 0, y + 1]
        if x == 15:
            q = q - wx[256 + y : 257 + y, :] * field[0, 17, y + 1]
        if y == 0:
            q = q - wym[r, :] * field[0, x + 1, 0]
        if y == 15:
            q = q - wyp[r, :] * field[0, x + 1, 17]
        if x in (0, 15) or y in (0, 15):
            image[x, y] = q
        return q

    for x in range(16):
        for y in range(0, 16, 2) if x in (0, 15) else (0, 14):
            pack_pair(1, x, y, rim_row(x, y), rim_row(x, y + 1))
    gather(1)
    for n in range(7):
        a2a_out(1, n).start()

    def first_sums(x, carry):
        rz, zq = carry
        for y in range(16):
            v = field[0, x + 1, y + 1]
            rz = rz + load_row(x, y) * v
            zq = zq + image[x, y] * v
        return rz, zq

    ar_begin(0, 0, as_row(*lax.fori_loop(0, 16, first_sums, (zero, zero))))
    precondition(1)
    if n_height > 1:
        pl.semaphore_wait(far_sem, n_height - 1)
    ar_begin(0, 1, ar_end(0, 0, add))
    setup_phase_part()
    pack_edge_weights()
    scatter(1)
    start_all(halo_copies(1))
    total = ar_end(0, 1, add)
    rz1 = from_row(total, 0)
    zq1 = from_row(total, 1)
    alpha1 = rz1 / zq1

    def local_second(x, carry, low, high):
        rz, zaz, zq = carry
        for y in range(16):
            w, u = local(1, x, y, low, high)
            q1 = image[x, y]
            z2 = field[0, x + 1, y + 1] - alpha1 * w
            rz = rz + (load_row(x, y) - alpha1 * q1) * z2
            zaz = zaz + z2 * (q1 - alpha1 * u)
            zq = zq + z2 * q1
        return rz, zaz, zq

    rz, zaz, zq = over_planes(local_second, (zero, zero, zero))
    receive_depth(1)
    receive_all(halo_copies(1)[:4])

    def second_direction(x, y):
        return field[0, x + 1, y + 1] - alpha1 * field[1, x + 1, y + 1]

    outer = zero
    for y in range(16):
        outer = outer + second_direction(0, y) * (wx[y : y + 1, :] * field[1, 0, y + 1])
        outer = outer + second_direction(15, y) * (wx[256 + y : 257 + y, :] * field[1, 17, y + 1])
        outer = outer + second_direction(y, 0) * (wym[16 * y : 16 * y + 1, :] * field[1, y + 1, 0])
        outer = outer + second_direction(y, 15) * (
            wyp[16 * y + 15 : 16 * y + 16, :] * field[1, y + 1, 17]
        )
    for g in range(4):
        outer = outer + (hz_s[0, g] - alpha1 * hz_s[1, g]) * (wzp[g] * hz_m[1, g])
    ar_begin(1, 0, as_row(rz, zaz + alpha1 * outer, zq))

    def quadratic(x, _):
        hz0 = hz_m[0, (x % 8) // 2]
        hz1 = hz_m[1, (x % 8) // 2]
        for y in range(16):
            r = pl.ds(x * 16 + y, 1)
            z, w = field[0, x + 1, y + 1], field[1, x + 1, y + 1]
            zz = zw = ww = zero
            for weight, near_z, near_w in (
                (wx[r, :], field[0, x, y + 1], field[1, x, y + 1]),
                (wx[pl.ds(x * 16 + 16 + y, 1), :], field[0, x + 2, y + 1], field[1, x + 2, y + 1]),
                (wym[r, :], field[0, x + 1, y], field[1, x + 1, y]),
                (wyp[r, :], field[0, x + 1, y + 2], field[1, x + 1, y + 2]),
                (wze[r, :], side_values(hz0, x, y), side_values(hz1, x, y)),
            ):
                solid = weight > 0.0
                dz = jnp.where(solid, z - near_z, 0.0)
                dw = jnp.where(solid, w - near_w, 0.0)
                zz, zw, ww = zz + dz * dz, zw + dz * dw, ww + dw * dw
            solid = wzl[r, :] > 0.0
            dz = jnp.where(solid, z - pltpu.roll(z, 127, 1), 0.0)
            dw = jnp.where(solid, w - pltpu.roll(w, 127, 1), 0.0)
            uz, uw = pltpu.roll(dz, 1, 1), pltpu.roll(dw, 1, 1)
            quads[0, x, y] = zz + dz * dz + uz * uz
            quads[1, x, y] = zw + dz * dw + uz * uw
            quads[2, x, y] = ww + dw * dw + uw * uw
        return 0

    lax.fori_loop(0, 8, quadratic, 0)
    ar_begin(1, 1, ar_end(1, 0, add))
    lax.fori_loop(8, 16, quadratic, 0)
    for it in range(2):
        for n in range(7):
            a2a_out(it, n).wait_send()
            a2a_back(it, n).wait_send()
        sent_all(halo_copies(it))
    total = ar_end(1, 1, add)
    rz2 = from_row(total, 0)
    zaz = from_row(total, 1)
    zq2 = from_row(total, 2)
    beta = rz2 / rz1
    alpha2 = rz2 / (zaz + beta * (2.0 * zq2 + beta * zq1))
    on_z = alpha1 + alpha2 * (1.0 + beta)
    on_w = -alpha2 * alpha1
    on_zz, on_zw, on_ww = on_z * on_z, 2.0 * on_z * on_w, on_w * on_w

    def sensitivities(x, peak):
        for h in range(2):
            energy = load_sums(
                [
                    on_zz * quads[0, x, 8 * h + y]
                    + on_zw * quads[1, x, 8 * h + y]
                    + on_ww * quads[2, x, 8 * h + y]
                    for y in range(8)
                ]
            )
            at = pl.multiple_of(x * 16, 16) + 8 * h
            s = rate[pl.ds(at, 8), :] * energy
            sens[pl.ds(at, 8), :] = s
            ext[3, pl.ds(at + 16, 8), :] = inverse * s
            peak = jnp.maximum(peak, -s)
        return peak

    peak = lax.fori_loop(0, 16, sensitivities, zero)
    ar_begin(2, 0, jnp.max(peak, axis=0, keepdims=True))
    small_faces(3)
    start_all(small_copies(3))

    def form(x, _):
        for y in range(16):
            dx[pl.ds(x * 16 + y, 8, stride=PITCH), :] = (
                on_z * field[0, x + 1, y + 1] + on_w * field[1, x + 1, y + 1]
            )
        return 0

    lax.fori_loop(0, 16, form, 0)
    ar_begin(2, 1, ar_end(2, 0, jnp.maximum))
    receive_all(small_copies(3))
    small_merge(3)

    def slopes(x, _):
        slope[rows_of(x), :] = small_block(3, x) + (interface_weight * inverse) * small_sum(3, x)

    unrolled(16, 4, slopes)
    for e in range(3):
        sent_all(small_copies(e))
    for k in range(2):
        for stage in range(2):
            for c in ar_copies(k, stage):
                c.wait_send()
    peak = jnp.max(ar_end(2, 1, jnp.maximum), axis=1, keepdims=True)
    scale = jnp.broadcast_to(1.0 / (peak + epsilon_peak), (8, 128))
    for n in range(32):
        at = slice(8 * n, 8 * n + 8)
        nxt[at, :] = hpart[at, :] - slope[at, :] * scale

    sent_all(small_copies(3))
    for stage in range(2):
        for c in ar_copies(2, stage):
            c.wait_send()


def deliver(dx, sens, nxt, disp_hbm, sens_hbm, next_hbm, sem):
    copies = [
        pltpu.make_async_copy(
            dx.at[pl.ds(l * PITCH, 256)], disp_hbm.at[pl.ds(l * 256, 256)], sem.at[l]
        )
        for l in range(8)
    ]
    copies.append(pltpu.make_async_copy(sens, sens_hbm, sem.at[8]))
    copies.append(pltpu.make_async_copy(nxt, next_hbm, sem.at[9]))
    for c in copies:
        c.start()
    for c in copies:
        c.wait()


def solution(mesh):
    sizes = tuple(mesh.shape[a] for a in AXES)
    dma = pltpu.SemaphoreType.DMA
    vmem = pltpu.VMEM

    def local(load, phase, void, owner, precond):
        vmem_space = pl.BlockSpec(memory_space=pltpu.VMEM)
        hbm_space = pl.BlockSpec(memory_space=pltpu.HBM)
        results = pl.pallas_call(
            functools.partial(kernel, sizes),
            name="design_step",
            out_shape=(
                jax.ShapeDtypeStruct((8 * PITCH, 128), F32),
                jax.ShapeDtypeStruct((256, 128), F32),
                jax.ShapeDtypeStruct((256, 128), F32),
            ),
            in_specs=[hbm_space] * 5,
            out_specs=(vmem_space,) * 3,
            scratch_shapes=[
                vmem((8 * PITCH, 128), F32),
                vmem((2, 2, 16), jnp.int32),
                vmem((2, 2, 16), jnp.int32),
                vmem((16, 512, 512), BF16),
                vmem((256, 512), BF16),
                vmem((256, 128), BF16),
                vmem((8, 128), F32),
                vmem((512, 1024), BF16),
                vmem((512, 256), BF16),
                vmem((8, 16, 512), BF16),
                vmem((8, 32, 512), BF16),
                vmem((8, 16, 512), BF16),
                vmem((8, 32, 512), BF16),
                vmem((2, 8, 16, 512), F32),
                vmem((2, 8, 16, 512), F32),
                vmem((2, 18, 18, 8, 128), F32),
                vmem((16, 16, 8, 128), F32),
                vmem((3, 16, 16, 8, 128), F32),
                vmem((2, 4, 8, 128), F32),
                vmem((2, 2, 4, 8, 128), F32),
                vmem((2, 4, 8, 128), F32),
                vmem((4, 8, 128), F32),
                vmem((4, 288, 128), F32),
                vmem((4, 3, 16, 128), F32),
                vmem((4, 3, 16, 128), F32),
                vmem((4, 8, 128), F32),
                vmem((256, 128), F32),
                vmem((272, 128), F32),
                vmem((256, 128), F32),
                vmem((256, 128), F32),
                vmem((256, 128), F32),
                vmem((256, 128), F32),
                vmem((256, 128), F32),
                vmem((256, 128), F32),
                vmem((256, 128), F32),
                vmem((256, 128), F32),
                vmem((3, 2, 1, 128), F32),
                vmem((3, 22, 1, 128), F32),
                dma((11,)),
                dma((8,)),
                dma((2, 7)),
                dma((2, 7)),
                dma((2, 7)),
                dma((2, 7)),
                dma((2, 6)),
                dma((2, 6)),
                dma((4, 6)),
                dma((4, 6)),
                dma((3, 22)),
                dma((3, 22)),
                pltpu.SemaphoreType.REGULAR,
            ],
            compiler_params=pltpu.CompilerParams(
                collective_id=0, has_side_effects=True, vmem_limit_bytes=48 * 2**20
            ),
        )(*(
            pltpu.with_memory_space_constraint(a, pltpu.HBM)
            for a in (load.reshape(2048, 128), phase.reshape(256, 128), void, owner, precond)
        ))
        disp, sens, nxt = pl.pallas_call(
            deliver,
            name="deliver",
            out_shape=(
                jax.ShapeDtypeStruct((2048, 128), F32),
                jax.ShapeDtypeStruct((256, 128), F32),
                jax.ShapeDtypeStruct((256, 128), F32),
            ),
            in_specs=[pl.BlockSpec(memory_space=pl.ANY)] * 3,
            out_specs=(hbm_space,) * 3,
            scratch_shapes=[dma((10,))],
            compiler_params=pltpu.CompilerParams(vmem_limit_bytes=2**20),
        )(*results)
        return (
            disp.reshape(8, 16, 16, 128),
            sens.reshape(16, 16, 128),
            nxt.reshape(16, 16, 128),
        )

    return jax.shard_map(
        local,
        mesh=mesh,
        in_specs=(P(None, *AXES), P(*AXES), P(*AXES), P(*AXES), P(AXES, None, None)),
        out_specs=(P(None, *AXES), P(*AXES), P(*AXES)),
        check_vma=False,
    )
```

```python
import functools

import jax
import jax.numpy as jnp
from jax import lax
from jax.experimental import pallas as pl
from jax.experimental.pallas import tpu as pltpu
from jax.sharding import PartitionSpec as P

AXES = ("span", "height", "depth")
MESH = pl.DeviceIdType.MESH
F32 = jnp.float32
BF16 = jnp.bfloat16

void_stiffness = 0.001
spring_rate = 0.05
time_step = 0.5
interface_weight = 0.5
epsilon_peak = 1e-06
inverse = 1.0 / (1.0 / time_step + 6.0 * interface_weight)

PITCH = 264

PARTNERS = ((0, 1), (1, 0), (3, 0), (1, 1), (3, 1), (2, 0), (2, 1))


def block_transpose(rows):
    lane_block = lax.broadcasted_iota(jnp.int32, (8, 128), 1) // 8
    rows = [pltpu.roll(r, 8 * t, 1) if t else r for t, r in enumerate(rows)]
    for bit in (1, 2, 4, 8):
        taken = (lane_block % (2 * bit)) >= bit
        rows = [jnp.where(taken, rows[(t + bit) % 16], rows[t]) for t in range(16)]
    out = []
    for s in range(16):
        r = rows[(16 - s) % 16]
        out.append(pltpu.roll(r, 128 - 8 * s, 1) if s else r)
    return out


def kernel(
    sizes,
    load_hbm, phase_hbm, void_hbm, owner_hbm, precond_hbm,
    dx, sens, nxt,
    load_v, void_v, owner_v, pre_v, sel, ez, mrow, lb, gbuf,
    send_a0, send_a1, recv_a0, recv_a1, send_r, recv_r, field, image, quads, hz_s, hz_r, hz_m, wzp,
    ext, sf_s, sf_r, sf_m, dco, wx, wyp, wym, wzl, wze, base, hpart, slope, rate, ar_s, ar_r,
    in_sem, pre_sem, a2a_ss, a2a_rs, ret_ss, ret_rs, halo_ss, halo_rs,
    sf_ss, sf_rs, ar_ss, ar_rs, far_sem,
):
    n_span, n_height, n_depth = sizes
    send_a, recv_a = (send_a0, send_a1), (recv_a0, recv_a1)
    S, H, D = (lax.axis_index(a) for a in AXES)
    yy, core = S // 2, S % 2
    lane = lax.broadcasted_iota(jnp.int32, (8, 128), 1)

    def towards(dy, dc):
        return lax.rem(yy + dy, 4) * 2 + (1 - core if dc else core)

    def back(dy, dc):
        return lax.rem(yy + 4 - dy, 4) * 2 + (1 - core if dc else core)

    load_in = [
        pltpu.make_async_copy(
            load_hbm.at[pl.ds(l * 256, 256)], load_v.at[pl.ds(l * PITCH, 256)], in_sem.at[l]
        )
        for l in range(8)
    ]
    void_in = pltpu.make_async_copy(void_hbm, void_v, in_sem.at[8])
    owner_in = pltpu.make_async_copy(owner_hbm, owner_v, in_sem.at[9])
    phase_in = pltpu.make_async_copy(phase_hbm, ext.at[1, pl.ds(16, 256)], in_sem.at[10])
    void_in.start()
    owner_in.start()
    for c in load_in:
        c.start()
    phase_in.start()

    barrier = pltpu.get_barrier_semaphore()
    for dy, dc in PARTNERS:
        pl.semaphore_signal(barrier, 1, device_id={"span": towards(dy, dc)}, device_id_type=MESH)
    for d in range(1, n_height):
        pl.semaphore_signal(
            barrier, 1, device_id={"height": lax.rem(H + d, n_height)}, device_id_type=MESH
        )
    for d in range(1, n_depth):
        pl.semaphore_signal(
            barrier, 1, device_id={"depth": lax.rem(D + d, n_depth)}, device_id_type=MESH
        )

    sources = [S] + [back(dy, dc) for dy, dc in PARTNERS]
    pre_in = [
        pltpu.make_async_copy(
            precond_hbm.at[pl.ds(src * 2, 2)], pre_v.at[pl.ds(src * 2, 2)], pre_sem.at[n]
        )
        for n, src in enumerate(sources)
    ]
    lane_row = lax.broadcasted_iota(jnp.int32, (1, 128), 1)

    def plan():
        void_in.wait()
        owner_in.wait()
        o_row = lax.broadcasted_iota(jnp.int32, (8, 16), 0)
        onehots = []
        for bx in range(2):
            own2, solid2 = owner_v[bx], 1 - void_v[bx]
            for by in range(2):
                own_row = jnp.broadcast_to(own2[by : by + 1, :], (8, 16))
                sol_row = jnp.broadcast_to(solid2[by : by + 1, :], (8, 16))
                onehots.append(jnp.where((own_row == o_row) & (sol_row == 1), 1.0, 0.0))
        onehot = jnp.concatenate(onehots, axis=0)
        b_row = lax.broadcasted_iota(jnp.int32, (16, 128), 0)
        b_lane = lax.broadcasted_iota(jnp.int32, (16, 128), 1) // 8
        spread = jnp.concatenate(
            [
                jnp.where(b_row == b_lane, 1.0, 0.0),
                jnp.where(b_row < b_lane, 1.0, 0.0),
                jnp.ones((16, 128), F32),
            ],
            axis=1,
        )
        counted = jnp.dot(onehot, spread, preferred_element_type=F32)
        o_col = lax.broadcasted_iota(jnp.int32, (8, 128), 0).astype(F32)
        row_id = lax.broadcasted_iota(jnp.int32, (128, 128), 0).astype(F32)
        previous = jnp.zeros((8, 128), F32)
        edge = jnp.full((1, 128), -1.0, F32)
        for c in range(4):
            here = counted[c * 8 : c * 8 + 8, 0:128]
            before = counted[c * 8 : c * 8 + 8, 128:256] + previous
            previous = previous + counted[c * 8 : c * 8 + 8, 256:384]
            solid = jnp.sum(here, axis=0, keepdims=True)
            slot = jnp.sum(here * (2.0 * o_col + before), axis=0, keepdims=True)
            code = jnp.where(solid > 0.5, slot * 8.0 + (lane_row % 8).astype(F32), -1.0)
            mrow[c : c + 1, :] = solid
            picked = jnp.where(row_id == code, 1.0, 0.0).astype(BF16)
            sel[0:128, c * 128 : (c + 1) * 128] = picked
            sel[128:256, c * 128 : (c + 1) * 128] = picked
            edge = jnp.where(lane_row % 8 == 2 * c, jnp.broadcast_to(code[:, 127:128], (1, 128)), edge)
            edge = jnp.where(lane_row % 8 == 2 * c + 1, jnp.broadcast_to(code[:, 0:1], (1, 128)), edge)
        picked = jnp.where(row_id == edge, 1.0, 0.0).astype(BF16)
        ez[0:128, :] = picked
        ez[128:256, :] = picked

    def halo_copies(it):
        f = field.at[it]
        inner = pl.ds(1, 16)
        copies = []
        for n, (axis, idx, size, src, dst) in enumerate(
            (
                ("span", S, n_span, f.at[16, inner], f.at[0, inner]),
                ("span", S, n_span, f.at[1, inner], f.at[17, inner]),
                ("height", H, n_height, f.at[inner, 16], f.at[inner, 0]),
                ("height", H, n_height, f.at[inner, 1], f.at[inner, 17]),
                ("depth", D, n_depth, hz_s.at[it], hz_r.at[it, 0]),
                ("depth", D, n_depth, hz_s.at[it], hz_r.at[it, 1]),
            )
        ):
            copies.append((axis, idx, size, n % 2, src, dst, halo_ss.at[it, n], halo_rs.at[it, n]))
        return copies

    def small_copies(e):
        f = ext.at[e]
        copies = []
        for n, (axis, idx, size, src, dst) in enumerate(
            (
                ("span", S, n_span, f.at[pl.ds(256, 16)], f.at[pl.ds(0, 16)]),
                ("span", S, n_span, f.at[pl.ds(16, 16)], f.at[pl.ds(272, 16)]),
                ("height", H, n_height, sf_s.at[e, 1], sf_r.at[e, 0]),
                ("height", H, n_height, sf_s.at[e, 0], sf_r.at[e, 1]),
                ("depth", D, n_depth, sf_s.at[e, 2, pl.ds(0, 8)], sf_r.at[e, 2, pl.ds(0, 8)]),
                ("depth", D, n_depth, sf_s.at[e, 2, pl.ds(0, 8)], sf_r.at[e, 2, pl.ds(8, 8)]),
            )
        ):
            copies.append((axis, idx, size, n % 2, src, dst, sf_ss.at[e, n], sf_rs.at[e, n]))
        return copies

    def make(copy):
        axis, idx, size, direction, src, dst, ss, rs = copy
        target = idx + 1 if direction == 0 else idx - 1
        return pltpu.make_async_remote_copy(
            src_ref=src, dst_ref=dst, send_sem=ss, recv_sem=rs,
            device_id={axis: lax.rem(target + size, size)}, device_id_type=MESH,
        )

    def sends(copy):
        _, idx, size, direction = copy[:4]
        return idx < size - 1 if direction == 0 else idx > 0

    def receives(copy):
        _, idx, size, direction = copy[:4]
        return idx > 0 if direction == 0 else idx < size - 1

    def start_all(copies):
        for copy in copies:
            if copy[2] > 1:
                pl.when(sends(copy))(lambda copy=copy: make(copy).start())

    def receive_all(copies):
        for copy in copies:
            if copy[2] > 1:
                pl.when(receives(copy))(lambda copy=copy: make(copy).wait_recv())

    def sent_all(copies):
        for copy in copies:
            if copy[2] > 1:
                pl.when(sends(copy))(lambda copy=copy: make(copy).wait_send())

    def span_copy(src, dst, ss, rs, partner):
        return pltpu.make_async_remote_copy(
            src_ref=src, dst_ref=dst, send_sem=ss, recv_sem=rs,
            device_id={"span": partner}, device_id_type=MESH,
        )

    def a2a_out(it, n):
        to = towards(*PARTNERS[n])
        return span_copy(
            send_a[it].at[to], recv_a[it].at[S], a2a_ss.at[it, n], a2a_rs.at[it, n], to
        )

    def a2a_back(it, n):
        to = back(*PARTNERS[n])
        return span_copy(
            send_r.at[it, to], recv_r.at[it, S], ret_ss.at[it, n], ret_rs.at[it, n], to
        )

    plane = [(h, d) for h in range(n_height) for d in range(n_depth) if h or d]

    def ar_copies(k, stage):
        copies = []
        for n, p in enumerate(PARTNERS if stage == 0 else plane):
            at = n + 7 * stage
            if stage == 0:
                target = {"span": towards(*p)}
            else:
                target = {
                    "height": lax.rem(H + p[0], n_height),
                    "depth": lax.rem(D + p[1], n_depth),
                }
            copies.append(
                pltpu.make_async_remote_copy(
                    src_ref=ar_s.at[k, stage], dst_ref=ar_r.at[k, at],
                    send_sem=ar_ss.at[k, at], recv_sem=ar_rs.at[k, at],
                    device_id=target, device_id_type=MESH,
                )
            )
        return copies

    def ar_begin(k, stage, value):
        ar_s[k, stage] = value
        for c in reversed(ar_copies(k, stage)):
            c.start()

    def ar_end(k, stage, combine):
        copies = ar_copies(k, stage)
        for c in copies:
            c.wait_recv()
        total = ar_s[k, stage]
        for n in range(len(copies)):
            total = combine(total, ar_r[k, 7 * stage + n])
        return total

    def pack_pair(it, x, y, upper, lower):
        both = jnp.concatenate([upper, lower], axis=0)
        high = both.astype(BF16)
        if isinstance(x, tuple):
            bx, pair, side = x
            at = pl.multiple_of(pair * 128, 128) + side * 64 + (y % 8) * 8
            column = (bx * 2 + y // 8) * 128
        else:
            at, column = (x % 8) * 64 + (y % 8) * 8, ((x // 8) * 2 + y // 8) * 128
            if not isinstance(x, int):
                at, column = pl.multiple_of(at, 16), pl.multiple_of(column, 128)
        lb[pl.ds(at, 16), pl.ds(column, 128)] = high
        if it == 1:
            low = (both - high.astype(F32)).astype(BF16)
            lb[pl.ds(at, 16), pl.ds(column + 512, 128)] = low

    def gather(it):
        by_slot = (((1,), (1,)), ((), ()))
        for g in range(4):
            rows, lanes = slice(g * 128, g * 128 + 128), slice(g * 128, g * 128 + 128)
            chosen = lax.dot_general(
                lb[rows, 0:512], sel[0:128, :], by_slot, preferred_element_type=F32
            )
            if it == 1:
                chosen = chosen + lax.dot_general(
                    lb[rows, 512:1024], sel[0:128, :], by_slot, preferred_element_type=F32
                )
            slots = block_transpose([chosen[8 * t : 8 * t + 8, :] for t in range(16)])
            for o in range(8):
                pair = slots[2 * o : 2 * o + 2]
                if it == 0:
                    send_a[it][o, :, lanes] = jnp.concatenate(pair, axis=0).astype(BF16)
                    continue
                for rank in range(2):
                    high = pair[rank].astype(BF16).astype(F32)
                    send_a[it][o, rank * 16 : rank * 16 + 16, lanes] = jnp.concatenate(
                        [high, pair[rank] - high], axis=0
                    ).astype(BF16)

    def own_product(it, src, lhs, out):
        for rank in range(2):
            rows = lhs[...] if it == 0 else lhs[rank * 16 : rank * 16 + 16, :]
            result = jnp.dot(rows, pre_v[src * 2 + rank], preferred_element_type=F32)
            if it == 0:
                part = result[rank * 8 : rank * 8 + 8, :]
            else:
                part = result[0:8, :] + result[8:16, :]
            out[rank * 8 : rank * 8 + 8, :] = part

    def precondition(it):
        if it == 0:
            pre_in[0].wait()
        own_product(it, S, send_a[it].at[S], recv_r.at[it, S])
        for n in range(7):
            if it == 0:
                pre_in[n + 1].wait()
            elif n == 6:
                if n_height > 1:
                    pl.semaphore_wait(far_sem, n_height - 1)
                ar_begin(0, 1, ar_end(0, 0, add))
            src = sources[n + 1]
            a2a_out(it, n).wait_recv()
            own_product(it, src, recv_a[it].at[src], send_r.at[it, src])
            a2a_back(it, n).start()

    def scatter(it):
        for n in range(7):
            a2a_back(it, n).wait_recv()

        for g in range(4):
            slots = [
                recv_r[it, s // 2, (s % 2) * 8 : (s % 2) * 8 + 8, g * 128 : g * 128 + 128]
                for s in range(16)
            ]
            rows = block_transpose(slots)
            for t in range(0, 16, 2):
                both = jnp.concatenate([rows[t], rows[t + 1]], axis=0)
                high = both.astype(BF16)
                at = slice(g * 128 + 8 * t, g * 128 + 8 * t + 16)
                gbuf[at, 0:128] = high
                gbuf[at, 128:256] = (both - high.astype(F32)).astype(BF16)
            chunk = gbuf[g * 128 : g * 128 + 128, :]
            cells = jnp.dot(chunk, sel[...], preferred_element_type=F32)
            faces = jnp.dot(chunk, ez[...], preferred_element_type=F32)
            packed = jnp.zeros((8, 128), F32)
            for t in range(16):
                ii, j = t // 8, t % 8
                for c in range(4):
                    bx, by = c // 2, c % 2
                    field[it, 1 + 8 * bx + 2 * g + ii, 1 + 8 * by + j] = cells[
                        t * 8 : t * 8 + 8, c * 128 : (c + 1) * 128
                    ]
                packed = jnp.where(lane // 8 == t, faces[t * 8 : t * 8 + 8, :], packed)
            hz_s[it, g] = packed

    def merge(right, left):
        return jnp.where(lane % 2 == 0, pltpu.roll(right, 127, 1), pltpu.roll(left, 1, 1))

    def unrolled(count, step, body):
        def several(g, _):
            for k in range(step):
                body(g * step + k, 0)
            return 0

        lax.fori_loop(0, count // step, several, 0)

    def small_faces(e):
        for side, y in ((0, 0), (1, 15)):
            sf_s[e, side] = ext[e, pl.ds(16 + y, 16, stride=16), :]
        parts = [jnp.zeros((8, 128), F32)] * 4
        for n in range(32):
            rows = pltpu.roll(ext[e, 16 + 8 * n : 24 + 8 * n, :], 2 * n + 1, 1)
            parts[n % 4] = jnp.where(lane // 2 == n, rows, parts[n % 4])
        sf_s[e, 2, 0:8, :] = (parts[0] + parts[1]) + (parts[2] + parts[3])

    def small_merge(e):
        sf_m[e] = merge(sf_r[e, 2, 8:16, :], sf_r[e, 2, 0:8, :])

    sub16 = lax.broadcasted_iota(jnp.int32, (16, 128), 0)
    lane16 = lax.broadcasted_iota(jnp.int32, (16, 128), 1)

    def small_block(e, x):
        return ext[e, pl.ds(pl.multiple_of(x * 16 + 16, 16), 16), :]

    def small_neighbours(e, x):
        mid = small_block(e, x)
        xp = ext[e, pl.ds(pl.multiple_of(x * 16 + 32, 16), 16), :]
        xm = ext[e, pl.ds(pl.multiple_of(x * 16, 16), 16), :]
        low = jnp.broadcast_to(sf_r[e, 0, pl.ds(x, 1), :], (16, 128))
        high = jnp.broadcast_to(sf_r[e, 1, pl.ds(x, 1), :], (16, 128))
        yp = jnp.where(sub16 == 15, high, pltpu.roll(mid, 15, 0))
        ym = jnp.where(sub16 == 0, low, pltpu.roll(mid, 1, 0))
        sides = jnp.concatenate(
            [pltpu.roll(sf_m[e], 127 - 2 * (2 * x + h), 1) for h in range(2)], axis=0
        )
        zp = jnp.where(lane16 == 127, sides, pltpu.roll(mid, 127, 1))
        zm = jnp.where(lane16 == 0, sides, pltpu.roll(mid, 1, 1))
        return xp, xm, yp, ym, zp, zm

    def small_sum(e, x):
        xp, xm, yp, ym, zp, zm = small_neighbours(e, x)
        return xp + xm + yp + ym + zp + zm

    def mask_block(x):
        bx = x // 8
        both = mrow[pl.ds(2 * bx, 2), :]
        return jnp.where(
            sub16 < 8,
            jnp.broadcast_to(both[0:1, :], (16, 128)),
            jnp.broadcast_to(both[1:2, :], (16, 128)),
        )

    def rows_of(x):
        return pl.ds(pl.multiple_of(x * 16, 16), 16)

    def clear_halos():
        zero_plane = jnp.zeros((16, 8, 128), F32)
        zero_face = jnp.zeros((16, 128), F32)

        def clear(cond, fn):
            pl.when(cond)(fn)

        def span_low():
            for it in range(2):
                field[it, 0, 1:17] = zero_plane
            for e in range(4):
                ext[e, 0:16, :] = zero_face

        def span_high():
            for it in range(2):
                field[it, 17, 1:17] = zero_plane
            for e in range(4):
                ext[e, 272:288, :] = zero_face

        def height_low():
            for it in range(2):
                field[it, 1:17, 0] = zero_plane
            for e in range(4):
                sf_r[e, 0] = zero_face

        def height_high():
            for it in range(2):
                field[it, 1:17, 17] = zero_plane
            for e in range(4):
                sf_r[e, 1] = zero_face

        def depth_low():
            for it in range(2):
                hz_r[it, 0] = jnp.zeros((4, 8, 128), F32)
            for e in range(4):
                sf_r[e, 2, 0:8, :] = jnp.zeros((8, 128), F32)

        def depth_high():
            for it in range(2):
                hz_r[it, 1] = jnp.zeros((4, 8, 128), F32)
            for e in range(4):
                sf_r[e, 2, 8:16, :] = jnp.zeros((8, 128), F32)

        clear(S == 0, span_low)
        clear(S == n_span - 1, span_high)
        clear(H == 0, height_low)
        clear(H == n_height - 1, height_high)
        clear(D == 0, depth_low)
        clear(D == n_depth - 1, depth_high)

    def setup_masked_stiffness():
        phase_in.wait()

        def body(x, _):
            p = small_block(1, x)
            stiff = void_stiffness + (1.0 - void_stiffness) * (p * p * p)
            m = mask_block(x)
            ext[0, pl.ds(pl.multiple_of(x * 16 + 16, 16), 16), :] = m * stiff
            rate[rows_of(x), :] = (-1.5 * (1.0 - void_stiffness)) * (p * p) * m

        unrolled(16, 4, body)
        for e in range(2):
            small_faces(e)
            start_all(small_copies(e))

    def setup_coefficients():
        for e in range(2):
            receive_all(small_copies(e))
            small_merge(e)

        def body(x, _):
            p = small_block(1, x)
            stiff = void_stiffness + (1.0 - void_stiffness) * (p * p * p)
            m = mask_block(x)
            half = 0.5 * m
            total = m * spring_rate
            w = []
            for near in small_neighbours(0, x):
                one = half * (jnp.where(near > 0.0, stiff, 0.0) + near)
                total = total + one
                w.append(one)
            at = rows_of(x)
            dco[at, :] = total
            wx[pl.ds(pl.multiple_of(x * 16 + 16, 16), 16), :] = w[0]
            wx[at, :] = w[1]
            wyp[at, :] = w[2]
            wym[at, :] = w[3]
            wzl[at, :] = jnp.where(lane16 == 127, 0.0, w[4])
            wze[at, :] = jnp.where(lane16 == 127, w[4], jnp.where(lane16 == 0, w[5], 0.0))
            b = p / time_step - 0.5 * p * (1.0 - p) * (1.0 - 2.0 * p)
            base[at, :] = b
            ext[2, pl.ds(pl.multiple_of(x * 16 + 16, 16), 16), :] = inverse * (
                b + interface_weight * small_sum(1, x)
            )

        unrolled(16, 4, body)
        small_faces(2)
        start_all(small_copies(2))

    def setup_phase_part():
        receive_all(small_copies(2))
        small_merge(2)

        def body(x, _):
            at = rows_of(x)
            hpart[at, :] = inverse * (base[at, :] + interface_weight * small_sum(2, x))

        unrolled(16, 4, body)

    def load_row(x, y):
        return load_v[pl.ds(x * 16 + y, 8, stride=PITCH), :]

    def side_values(source, x, y):
        n = ((x % 2) * 8 + y % 8) * 4 + (x // 8) * 2 + y // 8
        return pltpu.roll(source, 127 - 2 * n, 1)

    def local(it, x, y, low, high):
        r = pl.ds(x * 16 + y, 1)
        v = field[it, x + 1, y + 1]
        wz = wzl[r, :]
        q = dco[r, :] * v
        if low:
            q = q - wx[r, :] * field[it, x, y + 1]
        if high:
            q = q - wx[pl.ds(x * 16 + 16 + y, 1), :] * field[it, x + 2, y + 1]
        if y > 0:
            q = q - wym[r, :] * field[it, x + 1, y]
        if y < 15:
            q = q - wyp[r, :] * field[it, x + 1, y + 2]
        return v, q - wz * pltpu.roll(v, 127, 1) - pltpu.roll(wz * v, 1, 1)

    def over_planes(body, carry):
        carry = body(0, carry, False, True)
        carry = lax.fori_loop(1, 15, lambda x, c: body(x, c, True, True), carry)
        return body(15, carry, True, False)

    lane_row8 = jnp.broadcast_to(lane_row, (8, 128))
    sub8 = lax.broadcasted_iota(jnp.int32, (8, 128), 0)

    def as_row(*accumulated):
        packed = jnp.zeros((8, 128), F32)
        for n, a in enumerate(accumulated):
            packed = jnp.where(lane_row8 == 8 * n + sub8, jnp.sum(a, axis=1, keepdims=True), packed)
        return jnp.sum(packed, axis=0, keepdims=True)

    def from_row(row, n):
        own = jnp.where(lane_row8 == 8 * n + sub8, jnp.broadcast_to(row, (8, 128)), 0.0)
        return jnp.broadcast_to(jnp.sum(own, axis=1, keepdims=True), (8, 128))

    def receive_depth(it):
        receive_all(halo_copies(it)[4:])
        for g in range(4):
            hz_m[it, g] = merge(hz_r[it, 1, g], hz_r[it, 0, g])

    def pack_edge_weights():
        def body(g, _):
            packed = [jnp.zeros((8, 128), F32)] * 4
            for ii in range(2):
                for c in range(4):
                    x = 8 * (c // 2) + 2 * g + ii
                    for j in range(8):
                        n = (ii * 8 + j) * 4 + c
                        row = wze[pl.ds(x * 16 + 8 * (c % 2) + j, 1), :]
                        row = pltpu.roll(jnp.broadcast_to(row, (8, 128)), 2 * n + 1, 1)
                        packed[c] = jnp.where(lane // 2 == n, row, packed[c])
            wzp[g] = (packed[0] + packed[1]) + (packed[2] + packed[3])
            return 0

        lax.fori_loop(0, 4, body, 0)

    def load_sums(rows):
        first = sub8 < 4
        out = []
        for y in range(4):
            a, b = rows[y], rows[y + 4]
            out.append(jnp.where(first, a, b) + pltpu.roll(jnp.where(first, b, a), 4, 0))
        rows = out
        for half in (2, 1):
            first = (sub8 % (2 * half)) < half
            out = []
            for y in range(half):
                a, b = rows[y], rows[y + half]
                other = jnp.where(first, b, a)
                moved = jnp.where(
                    first, pltpu.roll(other, 8 - half, 0), pltpu.roll(other, half, 0)
                )
                out.append(jnp.where(first, a, b) + moved)
            rows = out
        return rows[0]

    zero = jnp.zeros((8, 128), F32)
    add = lambda a, b: a + b

    plan()
    for c in load_in:
        c.wait()
    for c in pre_in:
        c.start()

    def pack_load(x, _):
        for y in range(0, 16, 2):
            pack_pair(0, x, y, load_row(x, y), load_row(x, y + 1))
        return 0

    lax.fori_loop(0, 16, pack_load, 0)
    gather(0)
    pl.semaphore_wait(barrier, 7 + (n_height - 1) + (n_depth - 1))
    for n in range(7):
        a2a_out(0, n).start()
    for d in range(1, n_height):
        pl.semaphore_signal(
            far_sem, 1, device_id={"height": lax.rem(H + d, n_height)}, device_id_type=MESH
        )
    clear_halos()
    setup_masked_stiffness()
    precondition(0)
    setup_coefficients()
    scatter(0)
    start_all(halo_copies(0))

    def local_first(x, carry, low, high):
        for y in range(16):
            image[x, y] = local(0, x, y, low, high)[1]
        return carry

    over_planes(local_first, 0)
    receive_depth(0)

    def pack_inner(pair, _):
        sides = hz_m[0, pair]
        for bx in range(2):
            for side in range(2):
                x = 8 * bx + 2 * pair + side
                for y in range(0, 16, 2):
                    q = []
                    for k in range(2):
                        n = (side * 8 + (y + k) % 8) * 4 + bx * 2 + y // 8
                        edge = wze[pl.ds(pair * 32 + (8 * bx + side) * 16 + y + k, 1), :]
                        q.append(image[x, y + k] - edge * pltpu.roll(sides, 127 - 2 * n, 1))
                        image[x, y + k] = q[k]
                    pack_pair(1, (bx, pair, side), y, *q)
        return 0

    lax.fori_loop(0, 4, pack_inner, 0)
    receive_all(halo_copies(0)[:4])

    def rim_row(x, y):
        r = slice(16 * x + y, 16 * x + y + 1)
        q = image[x, y]
        if x == 0:
            q = q - wx[r, :] * field[0, 0, y + 1]
        if x == 15:
            q = q - wx[256 + y : 257 + y, :] * field[0, 17, y + 1]
        if y == 0:
            q = q - wym[r, :] * field[0, x + 1, 0]
        if y == 15:
            q = q - wyp[r, :] * field[0, x + 1, 17]
        if x in (0, 15) or y in (0, 15):
            image[x, y] = q
        return q

    for x in range(16):
        for y in range(0, 16, 2) if x in (0, 15) else (0, 14):
            pack_pair(1, x, y, rim_row(x, y), rim_row(x, y + 1))
    gather(1)
    for n in range(7):
        a2a_out(1, n).start()

    def first_sums(x, carry):
        rz, zq = carry
        for y in range(16):
            v = field[0, x + 1, y + 1]
            rz = rz + load_row(x, y) * v
            zq = zq + image[x, y] * v
        return rz, zq

    ar_begin(0, 0, as_row(*lax.fori_loop(0, 16, first_sums, (zero, zero))))
    precondition(1)
    setup_phase_part()
    pack_edge_weights()
    scatter(1)
    start_all(halo_copies(1))
    total = ar_end(0, 1, add)
    rz1 = from_row(total, 0)
    zq1 = from_row(total, 1)
    alpha1 = rz1 / zq1

    def local_second(x, carry, low, high):
        rz, zaz, zq = carry
        for y in range(16):
            w, u = local(1, x, y, low, high)
            q1 = image[x, y]
            z2 = field[0, x + 1, y + 1] - alpha1 * w
            rz = rz + (load_row(x, y) - alpha1 * q1) * z2
            zaz = zaz + z2 * (q1 - alpha1 * u)
            zq = zq + z2 * q1
        return rz, zaz, zq

    rz, zaz, zq = over_planes(local_second, (zero, zero, zero))
    receive_depth(1)
    receive_all(halo_copies(1)[:4])

    def second_direction(x, y):
        return field[0, x + 1, y + 1] - alpha1 * field[1, x + 1, y + 1]

    outer = zero
    for y in range(16):
        outer = outer + second_direction(0, y) * (wx[y : y + 1, :] * field[1, 0, y + 1])
        outer = outer + second_direction(15, y) * (wx[256 + y : 257 + y, :] * field[1, 17, y + 1])
        outer = outer + second_direction(y, 0) * (wym[16 * y : 16 * y + 1, :] * field[1, y + 1, 0])
        outer = outer + second_direction(y, 15) * (
            wyp[16 * y + 15 : 16 * y + 16, :] * field[1, y + 1, 17]
        )
    for g in range(4):
        outer = outer + (hz_s[0, g] - alpha1 * hz_s[1, g]) * (wzp[g] * hz_m[1, g])
    ar_begin(1, 0, as_row(rz, zaz + alpha1 * outer, zq))

    def quadratic(x, _):
        hz0 = hz_m[0, (x % 8) // 2]
        hz1 = hz_m[1, (x % 8) // 2]
        for y in range(16):
            r = pl.ds(x * 16 + y, 1)
            z, w = field[0, x + 1, y + 1], field[1, x + 1, y + 1]
            zz = zw = ww = zero
            for weight, near_z, near_w in (
                (wx[r, :], field[0, x, y + 1], field[1, x, y + 1]),
                (wx[pl.ds(x * 16 + 16 + y, 1), :], field[0, x + 2, y + 1], field[1, x + 2, y + 1]),
                (wym[r, :], field[0, x + 1, y], field[1, x + 1, y]),
                (wyp[r, :], field[0, x + 1, y + 2], field[1, x + 1, y + 2]),
                (wze[r, :], side_values(hz0, x, y), side_values(hz1, x, y)),
            ):
                solid = weight > 0.0
                dz = jnp.where(solid, z - near_z, 0.0)
                dw = jnp.where(solid, w - near_w, 0.0)
                zz, zw, ww = zz + dz * dz, zw + dz * dw, ww + dw * dw
            solid = wzl[r, :] > 0.0
            dz = jnp.where(solid, z - pltpu.roll(z, 127, 1), 0.0)
            dw = jnp.where(solid, w - pltpu.roll(w, 127, 1), 0.0)
            uz, uw = pltpu.roll(dz, 1, 1), pltpu.roll(dw, 1, 1)
            quads[0, x, y] = zz + dz * dz + uz * uz
            quads[1, x, y] = zw + dz * dw + uz * uw
            quads[2, x, y] = ww + dw * dw + uw * uw
        return 0

    lax.fori_loop(0, 8, quadratic, 0)
    ar_begin(1, 1, ar_end(1, 0, add))
    lax.fori_loop(8, 16, quadratic, 0)
    for it in range(2):
        for n in range(7):
            a2a_out(it, n).wait_send()
            a2a_back(it, n).wait_send()
        sent_all(halo_copies(it))
    total = ar_end(1, 1, add)
    rz2 = from_row(total, 0)
    zaz = from_row(total, 1)
    zq2 = from_row(total, 2)
    beta = rz2 / rz1
    alpha2 = rz2 / (zaz + beta * (2.0 * zq2 + beta * zq1))
    on_z = alpha1 + alpha2 * (1.0 + beta)
    on_w = -alpha2 * alpha1
    on_zz, on_zw, on_ww = on_z * on_z, 2.0 * on_z * on_w, on_w * on_w

    def sensitivities(x, peak):
        for h in range(2):
            energy = load_sums(
                [
                    on_zz * quads[0, x, 8 * h + y]
                    + on_zw * quads[1, x, 8 * h + y]
                    + on_ww * quads[2, x, 8 * h + y]
                    for y in range(8)
                ]
            )
            at = pl.multiple_of(x * 16, 16) + 8 * h
            s = rate[pl.ds(at, 8), :] * energy
            sens[pl.ds(at, 8), :] = s
            ext[3, pl.ds(at + 16, 8), :] = inverse * s
            peak = jnp.maximum(peak, -s)
        return peak

    peak = lax.fori_loop(0, 16, sensitivities, zero)
    ar_begin(2, 0, jnp.max(peak, axis=0, keepdims=True))
    small_faces(3)
    start_all(small_copies(3))

    def form(x, _):
        for y in range(16):
            dx[pl.ds(x * 16 + y, 8, stride=PITCH), :] = (
                on_z * field[0, x + 1, y + 1] + on_w * field[1, x + 1, y + 1]
            )
        return 0

    lax.fori_loop(0, 16, form, 0)
    ar_begin(2, 1, ar_end(2, 0, jnp.maximum))
    receive_all(small_copies(3))
    small_merge(3)

    def slopes(x, _):
        slope[rows_of(x), :] = small_block(3, x) + (interface_weight * inverse) * small_sum(3, x)

    unrolled(16, 4, slopes)
    for e in range(3):
        sent_all(small_copies(e))
    for k in range(2):
        for stage in range(2):
            for c in ar_copies(k, stage):
                c.wait_send()
    peak = jnp.max(ar_end(2, 1, jnp.maximum), axis=1, keepdims=True)
    scale = jnp.broadcast_to(1.0 / (peak + epsilon_peak), (8, 128))
    for n in range(32):
        at = slice(8 * n, 8 * n + 8)
        nxt[at, :] = hpart[at, :] - slope[at, :] * scale

    sent_all(small_copies(3))
    for stage in range(2):
        for c in ar_copies(2, stage):
            c.wait_send()


def deliver(dx, sens, nxt, disp_hbm, sens_hbm, next_hbm, sem):
    copies = [
        pltpu.make_async_copy(
            dx.at[pl.ds(l * PITCH, 256)], disp_hbm.at[pl.ds(l * 256, 256)], sem.at[l]
        )
        for l in range(8)
    ]
    copies.append(pltpu.make_async_copy(sens, sens_hbm, sem.at[8]))
    copies.append(pltpu.make_async_copy(nxt, next_hbm, sem.at[9]))
    for c in copies:
        c.start()
    for c in copies:
        c.wait()


def solution(mesh):
    sizes = tuple(mesh.shape[a] for a in AXES)
    dma = pltpu.SemaphoreType.DMA
    vmem = pltpu.VMEM

    def local(load, phase, void, owner, precond):
        vmem_space = pl.BlockSpec(memory_space=pltpu.VMEM)
        hbm_space = pl.BlockSpec(memory_space=pltpu.HBM)
        results = pl.pallas_call(
            functools.partial(kernel, sizes),
            name="design_step",
            out_shape=(
                jax.ShapeDtypeStruct((8 * PITCH, 128), F32),
                jax.ShapeDtypeStruct((256, 128), F32),
                jax.ShapeDtypeStruct((256, 128), F32),
            ),
            in_specs=[hbm_space] * 5,
            out_specs=(vmem_space,) * 3,
            scratch_shapes=[
                vmem((8 * PITCH, 128), F32),
                vmem((2, 2, 16), jnp.int32),
                vmem((2, 2, 16), jnp.int32),
                vmem((16, 512, 512), BF16),
                vmem((256, 512), BF16),
                vmem((256, 128), BF16),
                vmem((8, 128), F32),
                vmem((512, 1024), BF16),
                vmem((512, 256), BF16),
                vmem((8, 16, 512), BF16),
                vmem((8, 32, 512), BF16),
                vmem((8, 16, 512), BF16),
                vmem((8, 32, 512), BF16),
                vmem((2, 8, 16, 512), F32),
                vmem((2, 8, 16, 512), F32),
                vmem((2, 18, 18, 8, 128), F32),
                vmem((16, 16, 8, 128), F32),
                vmem((3, 16, 16, 8, 128), F32),
                vmem((2, 4, 8, 128), F32),
                vmem((2, 2, 4, 8, 128), F32),
                vmem((2, 4, 8, 128), F32),
                vmem((4, 8, 128), F32),
                vmem((4, 288, 128), F32),
                vmem((4, 3, 16, 128), F32),
                vmem((4, 3, 16, 128), F32),
                vmem((4, 8, 128), F32),
                vmem((256, 128), F32),
                vmem((272, 128), F32),
                vmem((256, 128), F32),
                vmem((256, 128), F32),
                vmem((256, 128), F32),
                vmem((256, 128), F32),
                vmem((256, 128), F32),
                vmem((256, 128), F32),
                vmem((256, 128), F32),
                vmem((256, 128), F32),
                vmem((3, 2, 1, 128), F32),
                vmem((3, 22, 1, 128), F32),
                dma((11,)),
                dma((8,)),
                dma((2, 7)),
                dma((2, 7)),
                dma((2, 7)),
                dma((2, 7)),
                dma((2, 6)),
                dma((2, 6)),
                dma((4, 6)),
                dma((4, 6)),
                dma((3, 22)),
                dma((3, 22)),
                pltpu.SemaphoreType.REGULAR,
            ],
            compiler_params=pltpu.CompilerParams(
                collective_id=0, has_side_effects=True, vmem_limit_bytes=48 * 2**20
            ),
        )(*(
            pltpu.with_memory_space_constraint(a, pltpu.HBM)
            for a in (load.reshape(2048, 128), phase.reshape(256, 128), void, owner, precond)
        ))
        disp, sens, nxt = pl.pallas_call(
            deliver,
            name="deliver",
            out_shape=(
                jax.ShapeDtypeStruct((2048, 128), F32),
                jax.ShapeDtypeStruct((256, 128), F32),
                jax.ShapeDtypeStruct((256, 128), F32),
            ),
            in_specs=[pl.BlockSpec(memory_space=pl.ANY)] * 3,
            out_specs=(hbm_space,) * 3,
            scratch_shapes=[dma((10,))],
            compiler_params=pltpu.CompilerParams(vmem_limit_bytes=2**20),
        )(*results)
        return (
            disp.reshape(8, 16, 16, 128),
            sens.reshape(16, 16, 128),
            nxt.reshape(16, 16, 128),
        )

    return jax.shard_map(
        local,
        mesh=mesh,
        in_specs=(P(None, *AXES), P(*AXES), P(*AXES), P(*AXES), P(AXES, None, None)),
        out_specs=(P(None, *AXES), P(*AXES), P(*AXES)),
        check_vma=False,
    )
```
